128 devices in a mesh: replica: 1, data: 16 (over z, y), model: 8 (over x, core).
Axes of the slice: x: 4, y: 4, z: 4, core: 2. Of those that a mesh axis runs over, the one named last changes fastest.
Arguments:
- x_in: bfloat16 [32, 768, 2048], P(('replica', 'data'), 'model')
- lengths: int32 [32], P(('replica', 'data'))
- norm_gain: bfloat16 [2, 2048], P(None, 'data')
- w_in: bfloat16 [2, 2048, 34816], P(None, 'data', 'model')
- w_kv: bfloat16 [2, 2048, 512], P(None, 'data')
- w_out: bfloat16 [2, 18432, 2048], P(None, 'model', 'data')
Outputs:
- output: bfloat16 [32, 768, 2048], P(('replica', 'data'), 'model')
All inputs are finite; a program needn't handle non-finite values.
Results may differ from the reference program's by a relative error of at most 0.02.
Values are sent between devices in bfloat16 or wider.
A program may use at most 1 GiB of HBM per device.

```python
import jax
import jax.numpy as jnp
from jax import lax

DATA = 16
MODEL = 8
BATCH_DEV = 2
SEQ_DEV = 96
D = 2048
HEADS = 8
HEAD = 256
FF = 16384
LAYERS = 2

BATCH = BATCH_DEV * DATA
SEQ = SEQ_DEV * MODEL
HEADS_LOC = HEADS // MODEL
Q_COLS = HEADS_LOC * HEAD
FF_LOC = FF // MODEL
IN_COLS = Q_COLS + 2 * FF_LOC
OUT_ROWS = Q_COLS + FF_LOC
MIN_LEN = SEQ // 8
EPS = 1e-6
NEG_BIG = -1e30


def setup_inputs(seed: int = 0, part: int = 0) -> dict:
    part_key = jax.random.fold_in(jax.random.key(seed), part)
    key_x, key_len, key_pick = jax.random.split(part_key, 3)
    x_in = jax.random.normal(key_x, (BATCH, SEQ, D), jnp.float32).astype(jnp.bfloat16)
    lengths = jax.random.randint(key_len, (BATCH,), MIN_LEN, SEQ + 1)
    pick_order = jax.random.permutation(key_pick, BATCH)
    lengths = lengths.at[pick_order[0]].set(SEQ).at[pick_order[1]].set(MIN_LEN).astype(jnp.int32)
    weight_keys = jax.random.split(jax.random.key(seed + 1), 4)
    norm_gain = 1.0 + 0.4 * jax.random.normal(weight_keys[0], (LAYERS, D), jnp.float32)
    in_scale = jnp.tile(jnp.where(jnp.arange(IN_COLS) < Q_COLS, 2.5, 1.0), MODEL) * D ** -0.5
    w_in = jax.random.normal(weight_keys[1], (LAYERS, D, MODEL * IN_COLS), jnp.float32) * in_scale
    w_kv = jax.random.normal(weight_keys[2], (LAYERS, D, 2 * HEAD), jnp.float32) * D ** -0.5
    out_scale = jnp.tile(jnp.where(jnp.arange(OUT_ROWS) < Q_COLS, 3.0, 1.0), MODEL) * (HEADS * HEAD + FF) ** -0.5
    w_out = jax.random.normal(weight_keys[3], (LAYERS, MODEL * OUT_ROWS, D), jnp.float32) * out_scale[:, None]
    return {'x_in': x_in, 'lengths': lengths, 'norm_gain': norm_gain.astype(jnp.bfloat16), 'w_in': w_in.astype(jnp.bfloat16), 'w_kv': w_kv.astype(jnp.bfloat16), 'w_out': w_out.astype(jnp.bfloat16)}


def layer_norm(hidden, norm_gain):
    values_f = hidden.astype(jnp.float32)
    row_mean = jnp.mean(values_f, axis=-1, keepdims=True)
    centered = values_f - row_mean
    row_var = jnp.mean(centered * centered, axis=-1, keepdims=True)
    return (centered * lax.rsqrt(row_var + EPS) * norm_gain.astype(jnp.float32)).astype(jnp.bfloat16)


def reference(x_in, lengths, norm_gain, w_in, w_kv, w_out):
    key_pos = jnp.arange(SEQ)

    def one_layer(hidden, weights):
        gain_l, w_in_l, w_kv_l, w_out_l = weights
        w_out_f = w_out_l.reshape(MODEL, OUT_ROWS, D).astype(jnp.float32)

        def per_row(row_args):
            x_row, length = row_args
            normed = layer_norm(x_row, gain_l)
            proj_out = jnp.dot(normed, w_in_l, preferred_element_type=jnp.float32).astype(jnp.bfloat16)
            proj_out = proj_out.reshape(MODEL, SEQ_DEV, MODEL, IN_COLS)
            kv_out = jnp.dot(normed, w_kv_l, preferred_element_type=jnp.float32).astype(jnp.bfloat16).astype(jnp.float32)
            key_vecs = kv_out[:, :HEAD]
            value_vecs = kv_out[:, HEAD:]
            valid = key_pos < length

            def per_block(blk_args):
                proj_blk, x_blk, block_idx = blk_args
                q_pos = block_idx * SEQ_DEV + jnp.arange(SEQ_DEV)
                allowed = (key_pos[None, :] <= q_pos[:, None]) & valid[None, :]
                queries = proj_blk[:, :, :Q_COLS].reshape(SEQ_DEV, MODEL, HEADS_LOC, HEAD).astype(jnp.float32)
                scores = jnp.einsum('tjhe,se->jhts', queries, key_vecs) * HEAD ** -0.5
                scores = jnp.where(allowed, scores, NEG_BIG)
                attn_prob = jax.nn.softmax(scores, axis=-1)
                attn_out = jnp.einsum('jhts,se->tjhe', attn_prob, value_vecs).astype(jnp.bfloat16)
                gate_pre = proj_blk[:, :, Q_COLS:Q_COLS + FF_LOC].astype(jnp.float32)
                up_proj = proj_blk[:, :, Q_COLS + FF_LOC:].astype(jnp.float32)
                mlp_out = (jax.nn.silu(gate_pre) * up_proj).astype(jnp.bfloat16)
                joined = jnp.concatenate([attn_out.reshape(SEQ_DEV, MODEL, Q_COLS), mlp_out], axis=-1).astype(jnp.float32)
                part_z = jnp.einsum('tjr,jrd->tjd', joined, w_out_f).astype(jnp.bfloat16).astype(jnp.float32)
                z_sum = jnp.sum(part_z, axis=1)
                return (x_blk.astype(jnp.float32) + z_sum).astype(jnp.bfloat16)

            blk_inputs = (proj_out, x_row.reshape(MODEL, SEQ_DEV, D), jnp.arange(MODEL))
            return lax.map(per_block, blk_inputs).reshape(SEQ, D)

        return lax.map(per_row, (hidden, lengths)), None

    y_out = lax.scan(one_layer, x_in, (norm_gain, w_in, w_kv, w_out))[0]
    return y_out
```

```python
import jax
import jax.numpy as jnp
from jax import lax
from jax.experimental import pallas as pl
from jax.experimental.pallas import tpu as pltpu
from jax.sharding import PartitionSpec as P

EPS = 1e-6
NEG_BIG = -1e30
MESH = pl.DeviceIdType.MESH
TILE = 512
RELS = (0, -1, 1, 2)
GROUPS = ((0, 'in'), (0, 'out'), (1, 'in'), (1, 'out'))
F32 = jnp.float32
BF16 = jnp.bfloat16
ORDER = ((0, 1), (4, 8), (2, 3), (5, 9), (6, 10), (7, 11), (12, 13), (14, 15))


def dot(a, b):
    return jnp.dot(a, b, preferred_element_type=F32)


def layer_kernel(ring, x_ref, gain_ref, valid_ref, win_ref, wout_ref, y_ref, winb, woutb,
                 h_all, joined, kvb, qb, wt, wo, zp, zrp, xh, xf, zs, hid, gbuf,
                 gsend, grecv, wsend, wrecv, asend, arecv, rsend, rrecv, bsem, tsem, osem):
    batch, blk, width = x_ref.shape
    shard = win_ref.shape[1]
    in_cols = win_ref.shape[2]
    out_rows = wout_ref.shape[1]
    head = qb.shape[-1]
    seq = h_all.shape[1]
    n_data = gbuf.shape[0]
    me = lax.axis_index('data')
    mi = lax.axis_index('model')
    yy = lax.rem(me, ring)
    zz = lax.div(me, ring)
    xx = lax.div(mi, 2)
    cc = lax.rem(mi, 2)

    def wrap(value, rel):
        return lax.rem(value + (rel + ring), ring)

    def data_at(ry, rz):
        return wrap(zz, rz) * ring + wrap(yy, ry)

    def dev_data(ry, rz):
        return {'data': data_at(ry, rz), 'model': mi}

    def dev_x(rx):
        return {'data': me, 'model': wrap(xx, rx) * 2 + cc}

    partner = {'data': me, 'model': xx * 2 + (1 - cc)}

    barrier = pltpu.get_barrier_semaphore()
    for ry in range(ring):
        for rz in range(ring):
            if ry or rz:
                pl.semaphore_signal(barrier, inc=1, device_id=dev_data(ry, rz), device_id_type=MESH)
    for dev in (dev_x(1), dev_x(-1), partner):
        pl.semaphore_signal(barrier, inc=1, device_id=dev, device_id_type=MESH)
    pl.semaphore_wait(barrier, n_data - 1 + 3)

    drains = []

    def remote(src, dst, ssem, rsem, dev):
        return pltpu.make_async_remote_copy(src_ref=src, dst_ref=dst, send_sem=ssem, recv_sem=rsem,
                                            device_id=dev, device_id_type=MESH)

    half_cols = in_cols // 2
    half_rows = out_rows // 2

    def unit(g, hf, rp, rq, part=None):
        layer, kind = GROUPS[g]
        s = data_at(rp, rq) if hf == 0 else data_at(rq, rp)
        if kind == 'in':
            n = shard if part is None else shard // 2
            start = pl.multiple_of(s * shard + (0 if part is None else part * n), 64)
            return winb.at[layer, pl.ds(start, n), pl.ds(hf * half_cols, half_cols)]
        n = half_rows if part is None else half_rows // 2
        return woutb.at[layer, s, pl.ds(hf * half_rows + (0 if part is None else part * n), n), :]

    def own(g, hf):
        layer, kind = GROUPS[g]
        if kind == 'in':
            return win_ref.at[layer, :, pl.ds(hf * half_cols, half_cols)]
        return wout_ref.at[layer, pl.ds(hf * half_rows, half_rows), :]

    def along(hf, primary, rel):
        on_y = (hf == 0) == primary
        return dev_data(rel, 0) if on_y else dev_data(0, rel)

    def send(g, hf, idx, rel, primary, to, part=None):
        def build():
            dst = unit(g, hf, rel[0], rel[1], part)
            src = own(g, hf) if rel == (0, 0) else dst
            return remote(src, dst, wsend.at[g, hf, idx], wrecv.at[g, hf, idx], along(hf, primary, to))
        build().start()
        drains.append(build)

    def spec(idx):
        if idx < 4:
            return ((-1, 0, None), (1, 0, None), (2, 0, 0), (2, 0, 1))[idx]
        return (RELS[idx % 4], (None, -1, 1, 2)[idx // 4], None)

    def start_group(g):
        for hf in (0, 1):
            send(g, hf, 0, (0, 0), True, 1)
            send(g, hf, 1, (0, 0), True, -1)
        for hf in (0, 1):
            send(g, hf, 4, (0, 0), False, 1)
            send(g, hf, 8, (0, 0), False, -1)

    def arrive(g, hf, idx):
        rp, rq, part = spec(idx)
        ref = unit(g, hf, rp, rq, part)
        remote(ref, ref, wsend.at[g, hf, idx], wrecv.at[g, hf, idx], along(hf, True, 1)).wait_recv()
        if idx == 0:
            send(g, hf, 2, (-1, 0), True, 1, 0)
            send(g, hf, 5, (-1, 0), False, 1)
            send(g, hf, 9, (-1, 0), False, -1)
        elif idx == 1:
            send(g, hf, 3, (1, 0), True, -1, 1)
            send(g, hf, 6, (1, 0), False, 1)
            send(g, hf, 10, (1, 0), False, -1)
        elif idx == 3:
            send(g, hf, 7, (2, 0), False, 1)
            send(g, hf, 11, (2, 0), False, -1)
        elif idx == 4:
            send(g, hf, 12, (0, -1), False, 1)
        elif idx == 5:
            send(g, hf, 13, (-1, -1), False, 1)
        elif idx == 10:
            send(g, hf, 14, (1, 1), False, -1)
        elif idx == 11:
            send(g, hf, 15, (2, 1), False, -1)

    events = []
    for g in range(len(GROUPS)):
        count = 0
        for pair in ORDER:
            for hf in (0, 1):
                for idx in pair:
                    if count == 24 and g + 1 < len(GROUPS):
                        events.append((g, lambda g=g: start_group(g + 1)))
                    events.append((g, lambda g=g, hf=hf, idx=idx: arrive(g, hf, idx)))
                    count += 1
    cursor = [0]

    def pump(n):
        for _ in range(n):
            if cursor[0] < len(events):
                events[cursor[0]][1]()
                cursor[0] += 1

    def pump_group(g):
        while cursor[0] < len(events) and events[cursor[0]][0] <= g:
            pump(1)

    gain_copies = []
    for ry in range(ring):
        for rz in range(ring):
            if ry or rz:
                k = rz * ring + ry
                copy = remote(gain_ref, gbuf.at[me], gsend.at[k], grecv.at[k], dev_data(ry, rz))
                copy.start()
                gain_copies.append((k, ry, rz))
    start_group(0)
    locals_ = []
    for layer in (0, 1):
        locals_.append(pltpu.make_async_copy(win_ref.at[layer], winb.at[layer, pl.ds(pl.multiple_of(me * shard, 128), shard), :], bsem.at[layer, 0]))
        locals_.append(pltpu.make_async_copy(wout_ref.at[layer], woutb.at[layer, me], bsem.at[layer, 1]))
    for copy in locals_:
        copy.start()
    hid[...] = x_ref[...]
    gbuf[me] = gain_ref[...]
    for k, ry, rz in gain_copies:
        src = gbuf.at[data_at(-ry, -rz)]
        remote(gain_ref, src, gsend.at[k], grecv.at[k], partner).wait()
    for copy in locals_:
        copy.wait()

    def block(rx, core, b=None):
        rows = pl.ds(pl.multiple_of((wrap(xx, rx) * 2 + core) * blk, 32), blk)
        return h_all.at[:, rows, :] if b is None else h_all.at[b, rows, :]

    def a_send(layer, idx, ref, dev, out):
        copy = remote(ref, ref, asend.at[layer, idx], arecv.at[layer, idx], dev)
        copy.start()
        out.append(copy)

    def a_wait(layer, idx, ref):
        remote(ref, ref, asend.at[layer, idx], arecv.at[layer, idx], partner).wait_recv()

    def norm_and_send(layer, out):
        rows = pl.ds(pl.multiple_of(mi * blk, 32), blk)
        for b in range(batch):
            values = hid[b].astype(F32)
            centered = values - jnp.mean(values, axis=-1, keepdims=True)
            var = jnp.mean(centered * centered, axis=-1, keepdims=True)
            normed = centered * lax.rsqrt(var + EPS)
            for i in range(n_data):
                cols = slice(i * shard, (i + 1) * shard)
                h_all[b, rows, cols] = (normed[:, cols] * gbuf[i, layer:layer + 1, :]).astype(BF16)
        mine = block(0, cc)
        a_send(layer, 0, mine, dev_x(1), out)
        a_send(layer, 1, mine, dev_x(-1), out)
        a_send(layer, 4, mine, partner, out)

    def gather_near(layer, out):
        a_wait(layer, 0, block(-1, cc))
        a_send(layer, 2, block(-1, cc, 0), dev_x(1), out)
        a_send(layer, 5, block(-1, cc), partner, out)
        a_wait(layer, 1, block(1, cc))
        a_send(layer, 3, block(1, cc, 1), dev_x(-1), out)
        a_send(layer, 6, block(1, cc), partner, out)

    def gather_far(layer, out):
        a_wait(layer, 2, block(2, cc, 0))
        a_send(layer, 7, block(2, cc, 0), partner, out)
        a_wait(layer, 3, block(2, cc, 1))
        a_send(layer, 8, block(2, cc, 1), partner, out)

    def gather_rest(layer):
        a_wait(layer, 4, block(0, 1 - cc))
        a_wait(layer, 5, block(-1, 1 - cc))
        a_wait(layer, 6, block(1, 1 - cc))
        a_wait(layer, 7, block(2, 1 - cc, 0))
        a_wait(layer, 8, block(2, 1 - cc, 1))

    n_mlp = (in_cols - 3 * head) // TILE
    m_rows = seq // 2

    def w_tile(layer, t, slot):
        return pltpu.make_async_copy(winb.at[layer, :, pl.ds(pl.multiple_of(t * TILE, TILE), TILE)], wt.at[slot], tsem.at[slot])

    def q_tile(layer, slot):
        return pltpu.make_async_copy(winb.at[layer, :, pl.ds((n_mlp + 1) * TILE, head)], wt.at[slot, :, pl.ds(0, head)], tsem.at[slot])

    def over_rows(fn):
        def body(i, carry):
            b = lax.div(i, 2)
            rows = pl.ds(pl.multiple_of(lax.rem(i, 2) * m_rows, m_rows), m_rows)
            fn(b, rows)
            return carry
        lax.fori_loop(0, 2 * batch, body, 0)

    def in_proj(layer, pumps):
        w_tile(layer, n_mlp, 0).start()
        q_tile(layer, 1).start()
        w_tile(layer, n_mlp, 0).wait()

        def do_kv(b, rows):
            kvb[b, rows, :] = dot(h_all[b, rows, :], wt[0]).astype(BF16)

        def do_q(b, rows):
            qb[b, rows, :] = dot(h_all[b, rows, :], wt[1, :, :head]).astype(BF16)

        over_rows(do_kv)
        w_tile(layer, 0, 0).start()
        pump(pumps)
        q_tile(layer, 1).wait()
        over_rows(do_q)
        pump(pumps)
        w_tile(layer, 1, 1).start()

        def body(t, carry):
            slot = lax.rem(t, 2)
            w_tile(layer, t, slot).wait()

            def do_mlp(b, rows):
                res = dot(h_all[b, rows, :], wt[slot])
                gate = res[:, :head].astype(BF16).astype(F32)
                up = res[:, head:].astype(BF16).astype(F32)
                cols = pl.ds(pl.multiple_of(head + t * head, head), head)
                joined[b, rows, cols] = (gate * jax.nn.sigmoid(gate) * up).astype(BF16)

            over_rows(do_mlp)

            @pl.when(t + 2 < n_mlp)
            def _():
                w_tile(layer, t + 2, slot).start()

            for k in range(n_mlp):
                @pl.when(t == k)
                def _():
                    pump(pumps)
            return carry

        lax.fori_loop(0, n_mlp, body, 0)

    def wo_copy(layer, s):
        return pltpu.make_async_copy(woutb.at[layer, s], wo.at[:, pl.ds(s * shard, shard)], osem.at[s])

    q_rows = 256

    def attention():
        def body(b, carry):
            for m in range(seq // q_rows):
                keys = (m + 1) * q_rows
                q = qb[b, m * q_rows:(m + 1) * q_rows, :]
                k = kvb[b, :keys, :head]
                s = lax.dot_general(q, k, (((1,), (1,)), ((), ())), preferred_element_type=F32) * head ** -0.5
                row = lax.broadcasted_iota(jnp.int32, (q_rows, keys), 0) + m * q_rows
                col = lax.broadcasted_iota(jnp.int32, (q_rows, keys), 1)
                allowed = (col <= row) & (valid_ref[b, :, :keys] > 0.5)
                s = jnp.where(allowed, s, NEG_BIG)
                e = jnp.exp(s - jnp.max(s, axis=-1, keepdims=True))
                p = e / jnp.sum(e, axis=-1, keepdims=True)
                o = dot(p, kvb[b, :keys, head:].astype(F32))
                joined[b, m * q_rows:(m + 1) * q_rows, :head] = o.astype(BF16)
            return carry
        lax.fori_loop(0, batch, body, 0)

    PAIRS = (2, 1, -1, 0)
    pair_rows = 2 * blk

    def out_proj(p):
        rows = pl.ds(pl.multiple_of(wrap(xx, PAIRS[p]) * pair_rows, 64), pair_rows)

        def body(n, carry):
            cols = pl.ds(pl.multiple_of(n * TILE, TILE), TILE)
            lhs = joined[:, rows, :].reshape(batch * pair_rows, out_rows)
            res = dot(lhs, wo[:, cols]).astype(BF16)
            zp[p, :, :, cols] = res.reshape(batch, pair_rows, TILE)
            return carry
        lax.fori_loop(0, width // TILE, body, 0)

    mine_rows = pl.ds(pl.multiple_of(cc * blk, 32), blk)
    other_rows = pl.ds(pl.multiple_of((1 - cc) * blk, 32), blk)

    def reduce_scatter(layer, out_ref, pumps):
        sends = []

        def r_send(idx, src, dst, dev):
            copy = remote(src, dst, rsend.at[layer, idx], rrecv.at[layer, idx], dev)
            copy.start()
            sends.append(copy)

        def r_wait(idx, dst):
            remote(dst, dst, rsend.at[layer, idx], rrecv.at[layer, idx], partner).wait_recv()

        def chunks(fn):
            for b in range(batch):
                def body(n, carry):
                    fn(b, pl.ds(pl.multiple_of(n * TILE, TILE), TILE))
                    return carry
                lax.fori_loop(0, width // TILE, body, 0)

        def base(p, b, cols):
            return zp[p, b, mine_rows, cols].astype(F32) + zrp[p, b, :, cols].astype(F32)

        def finish(p):
            r_wait(p, zrp.at[p])
            if p == 0:
                def fn(b, cols):
                    zs[0, b, :, cols] = base(0, b, cols).astype(BF16)
                chunks(fn)
                r_send(4, zs.at[0, 0], xh.at[0], dev_x(1))
                r_send(5, zs.at[0, 1], xh.at[1], dev_x(-1))
            elif p < 3:
                r_wait(3 + p, xh.at[p - 1])

                def fn(b, cols):
                    total = base(p, b, cols)
                    if b == p - 1:
                        total = total + xh[p - 1, :, cols].astype(F32)
                    zs[p, b, :, cols] = total.astype(BF16)
                chunks(fn)
                r_send(5 + p, zs.at[p], xf.at[p - 1], dev_x(1 if p == 1 else -1))
            else:
                r_wait(6, xf.at[0])
                r_wait(7, xf.at[1])

                def fn(b, cols):
                    total = base(3, b, cols) + xf[0, b, :, cols].astype(F32) + xf[1, b, :, cols].astype(F32)
                    out_ref[b, :, cols] = (hid[b, :, cols].astype(F32) + total).astype(BF16)
                chunks(fn)

        for p in range(4):
            out_proj(p)
            r_send(p, zp.at[p, :, other_rows, :], zrp.at[p], partner)
            pump(pumps)
            if p:
                finish(p - 1)
        pump(2 * pumps)
        finish(3)
        for copy in sends:
            copy.wait_send()

    for layer in (0, 1):
        a_sends = []
        norm_and_send(layer, a_sends)
        pump(8 if layer == 0 else 4)
        gather_near(layer, a_sends)
        pump(4)
        gather_far(layer, a_sends)
        pump(2)
        gather_rest(layer)
        pump_group(2 * layer)
        in_proj(layer, 3)
        for copy in a_sends:
            copy.wait_send()
        attention()
        pump_group(2 * layer + 1)
        for s in range(n_data):
            wo_copy(layer, s).start()
        for s in range(n_data):
            wo_copy(layer, s).wait()
        reduce_scatter(layer, hid if layer == 0 else y_ref, 2)

    for build in drains:
        build().wait_send()


def solution(mesh):
    batch_spec = ('replica', 'data')
    model_size = mesh.shape['model']
    n_data = mesh.shape['data']
    ring = 4
    assert model_size == 2 * ring and n_data == ring * ring

    def device_body(x_in, lengths, norm_gain, w_in, w_kv, w_out):
        batch, blk, width = x_in.shape
        layers, shard, in_cols = w_in.shape
        out_rows = w_out.shape[1]
        head = w_kv.shape[-1] // 2
        ff = in_cols - out_rows
        seq = blk * model_size
        valid = (jnp.arange(seq)[None, None, :] < lengths[:, None, None]).astype(F32)
        gain = jnp.zeros((8, shard), F32).at[:layers].set(norm_gain.astype(F32))
        gate = w_in[:, :, head:head + ff].reshape(layers, shard, ff // head, 1, head)
        up = w_in[:, :, head + ff:].reshape(layers, shard, ff // head, 1, head)
        gate_up = jnp.concatenate([gate, up], axis=3).reshape(layers, shard, 2 * ff)
        win = jnp.concatenate([gate_up, w_kv, w_in[:, :, :head]], axis=-1)
        total = win.shape[-1]
        vmem = pl.BlockSpec(memory_space=pltpu.VMEM)
        hbm = pl.BlockSpec(memory_space=pl.ANY)
        dma = pltpu.SemaphoreType.DMA
        y, _, _ = pl.pallas_call(
            lambda *refs: layer_kernel(ring, *refs),
            name='layers',
            out_shape=(
                jax.ShapeDtypeStruct(x_in.shape, BF16),
                jax.ShapeDtypeStruct((layers, width, total), BF16),
                jax.ShapeDtypeStruct((layers, n_data, out_rows, shard), BF16),
            ),
            in_specs=[vmem] * 5,
            out_specs=(vmem, hbm, hbm),
            scratch_shapes=[
                pltpu.VMEM((batch, seq, width), BF16),
                pltpu.VMEM((batch, seq, out_rows), BF16),
                pltpu.VMEM((batch, seq, 2 * head), BF16),
                pltpu.VMEM((batch, seq, head), BF16),
                pltpu.VMEM((2, width, TILE), BF16),
                pltpu.VMEM((out_rows, width), BF16),
                pltpu.VMEM((4, batch, 2 * blk, width), BF16),
                pltpu.VMEM((4, batch, blk, width), BF16),
                pltpu.VMEM((2, blk, width), BF16),
                pltpu.VMEM((2, batch, blk, width), BF16),
                pltpu.VMEM((3, batch, blk, width), BF16),
                pltpu.VMEM((batch, blk, width), BF16),
                pltpu.VMEM((n_data, 8, shard), F32),
                dma((n_data,)), dma((n_data,)),
                dma((4, 2, 16)), dma((4, 2, 16)),
                dma((2, 9)), dma((2, 9)),
                dma((2, 8)), dma((2, 8)),
                dma((2, 2)), dma((2,)), dma((n_data,)),
            ],
            compiler_params=pltpu.CompilerParams(
                collective_id=0, has_side_effects=True, vmem_limit_bytes=67043328),
            cost_estimate=pl.CostEstimate(flops=95_000_000_000, bytes_accessed=200_000_000, transcendentals=0),
        )(x_in, gain, valid, win, w_out)
        return y

    in_specs = (P(batch_spec, 'model', None), P(batch_spec), P(None, 'data'), P(None, 'data', 'model'), P(None, 'data', None), P(None, 'model', 'data'))
    return jax.shard_map(device_body, mesh=mesh, in_specs=in_specs, out_specs=P(batch_spec, 'model', None), check_vma=False)
```

```python
import jax
import jax.numpy as jnp
from jax import lax
from jax.experimental import pallas as pl
from jax.experimental.pallas import tpu as pltpu
from jax.sharding import PartitionSpec as P

EPS = 1e-6
NEG_BIG = -1e30
MESH = pl.DeviceIdType.MESH
TILE = 512
RELS = (0, -1, 1, 2)
KINDS = ('i0', 'i1', 'o')
GROUPS = tuple((layer, kind) for layer in (0, 1) for kind in KINDS)
F32 = jnp.float32
BF16 = jnp.bfloat16
ORDER = ((0, 1), (4, 8), (2, 3), (5, 9), (6, 10), (7, 11), (12, 13), (14, 15))
N_EVENTS = 32
START_NEXT = 20
OFFSETS = (0, 1.5, 7.5, 13.5, 19.5, 32, 38, 47)
BEGINS = (15, 72, 117, 165, 215, 259)
PHASES = ((34, 43, 76, 120, (144, 155, 160)), (206, 214, 219, 263, (290, 300, 304)))
STEP = 1.5
SUB = 128
BLOCKS = ((0, 0), (1, 0), (-1, 0), (0, 1), (0, -1), (1, 1), (-1, -1), (1, -1),
          (-1, 1), (2, 0), (0, 2), (2, -1), (-1, 2), (1, 2), (2, 1), (2, 2))
CHUNKS = ((0, 8), (8, 12), (12, 16))
CHUNK_EVENTS = (20, 28, 32)


def aligned(value, n):
    return value if isinstance(value, int) else pl.multiple_of(value, n)


def dot(a, b):
    return jnp.dot(a, b, preferred_element_type=F32)


def layer_kernel(ring, x_ref, len_ref, gain_in, win_ref, wkv_ref, wout_ref, y_ref, wi0, wi1, woutb,
                 gain_ref, h_all, joined, kvx, qb, wt, wo, zp, zrp, xh, xf, zs, hid, gbuf,
                 gsend, grecv, wsend, wrecv, asend, arecv, rsend, rrecv, bsem, tsem, osem):
    batch, blk, width = x_ref.shape
    shard = win_ref.shape[1]
    out_rows = wout_ref.shape[1]
    head = qb.shape[-1]
    kvc = kvx.shape[-1]
    seq = h_all.shape[1]
    n_data = gbuf.shape[0]
    ff = out_rows - head
    half_ff = ff // 2
    me = lax.axis_index('data')
    mi = lax.axis_index('model')
    yy = lax.rem(me, ring)
    zz = lax.div(me, ring)
    xx = lax.div(mi, 2)
    cc = lax.rem(mi, 2)

    def wrap(value, rel):
        return lax.rem(value + (rel + ring), ring)

    def data_at(ry, rz):
        return wrap(zz, rz) * ring + wrap(yy, ry)

    def dev_data(ry, rz):
        return {'data': data_at(ry, rz), 'model': mi}

    def dev_x(rx):
        return {'data': me, 'model': wrap(xx, rx) * 2 + cc}

    partner = {'data': me, 'model': xx * 2 + (1 - cc)}

    barrier = pltpu.get_barrier_semaphore()
    for ry in range(ring):
        for rz in range(ring):
            if ry or rz:
                pl.semaphore_signal(barrier, inc=1, device_id=dev_data(ry, rz), device_id_type=MESH)
    for dev in (dev_x(1), dev_x(-1), partner):
        pl.semaphore_signal(barrier, inc=1, device_id=dev, device_id_type=MESH)

    my_rows = pl.ds(pl.multiple_of(me * shard, 128), shard)
    locals_ = []

    def local(layer, i, src, dst):
        locals_.append(pltpu.make_async_copy(src, dst, bsem.at[layer, i]))

    for layer in (0, 1):
        kv_cols = pl.ds(pl.multiple_of(xx * kvc, 128), kvc)
        local(layer, 0, wkv_ref.at[layer, :, kv_cols], wi0.at[layer, my_rows, pl.ds(0, kvc)])
        local(layer, 1, win_ref.at[layer, :, pl.ds(0, head + half_ff)], wi0.at[layer, my_rows, pl.ds(kvc, head + half_ff)])
        local(layer, 2, win_ref.at[layer, :, pl.ds(head + ff, half_ff)], wi0.at[layer, my_rows, pl.ds(kvc + head + half_ff, half_ff)])
        local(layer, 3, win_ref.at[layer, :, pl.ds(head + half_ff, half_ff)], wi1.at[layer, my_rows, pl.ds(0, half_ff)])
        local(layer, 4, win_ref.at[layer, :, pl.ds(head + ff + half_ff, half_ff)], wi1.at[layer, my_rows, pl.ds(half_ff, half_ff)])
        local(layer, 5, wout_ref.at[layer], woutb.at[layer, me])
    for copy in locals_:
        copy.start()
    gain_ref[0:gain_in.shape[0], :] = gain_in[...].astype(F32)
    gbuf[me] = gain_ref[...]
    hid[...] = x_ref[...]
    pl.semaphore_wait(barrier, n_data - 1 + 3)

    drains = []

    def remote(src, dst, ssem, rsem, dev):
        return pltpu.make_async_remote_copy(src_ref=src, dst_ref=dst, send_sem=ssem, recv_sem=rsem,
                                            device_id=dev, device_id_type=MESH)

    half_in = shard // 2
    half_out = out_rows // 2

    def unit(g, hf, rp, rq, part=None):
        layer, kind = GROUPS[g]
        s = data_at(rp, rq) if hf == 0 else data_at(rq, rp)
        if kind == 'o':
            n = half_out if part is None else half_out // 2
            return woutb.at[layer, s, pl.ds(hf * half_out + (0 if part is None else part * n), n), :]
        n = half_in if part is None else half_in // 2
        start = pl.multiple_of(s * shard + (hf * half_in + (0 if part is None else part * n)), 32)
        return (wi0 if kind == 'i0' else wi1).at[layer, pl.ds(start, n), :]

    def along(hf, primary, rel):
        on_y = (hf == 0) == primary
        return dev_data(rel, 0) if on_y else dev_data(0, rel)

    def send(g, hf, idx, rel, primary, to, part=None):
        def build():
            ref = unit(g, hf, rel[0], rel[1], part)
            return remote(ref, ref, wsend.at[g, hf, idx], wrecv.at[g, hf, idx], along(hf, primary, to))
        build().start()
        drains.append(build)

    def spec(idx):
        if idx < 4:
            return ((-1, 0, None), (1, 0, None), (2, 0, 0), (2, 0, 1))[idx]
        return (RELS[idx % 4], (None, -1, 1, 2)[idx // 4], None)

    def start_group(g):
        for hf in (0, 1):
            send(g, hf, 0, (0, 0), True, 1)
            send(g, hf, 1, (0, 0), True, -1)
        for hf in (0, 1):
            send(g, hf, 4, (0, 0), False, 1)
            send(g, hf, 8, (0, 0), False, -1)

    def arrive(g, hf, idx):
        rp, rq, part = spec(idx)
        ref = unit(g, hf, rp, rq, part)
        remote(ref, ref, wsend.at[g, hf, idx], wrecv.at[g, hf, idx], along(hf, True, 1)).wait_recv()
        if idx < 2:
            send(g, hf, idx + 2, (rp, rq), True, -rp, idx)
        elif idx == 3:
            send(g, hf, 7, (rp, rq), False, 1)
            send(g, hf, 11, (rp, rq), False, -1)
        elif idx in (4, 5):
            send(g, hf, idx + 8, (rp, rq), False, 1)
        elif idx in (10, 11):
            send(g, hf, idx + 4, (rp, rq), False, -1)

    def turn_neighbors(g):
        for hf in (0, 1):
            for at in (1, 2):
                send(g, hf, at + 4, (RELS[at], 0), False, 1)
                send(g, hf, at + 8, (RELS[at], 0), False, -1)

    sequence = [(hf, idx) for pair in ORDER for hf in (0, 1) for idx in pair]
    cursor = [0]

    def pump(n):
        for _ in range(n):
            g, k = divmod(cursor[0], N_EVENTS)
            if g < len(GROUPS):
                if k == START_NEXT and g + 1 < len(GROUPS):
                    start_group(g + 1)
                arrive(g, *sequence[k])
                if k == 3:
                    turn_neighbors(g)
                cursor[0] += 1

    def due(n):
        g, k = divmod(n, N_EVENTS)
        return BEGINS[g] + OFFSETS[k // 4]

    def pump_until(time):
        while cursor[0] < len(GROUPS) * N_EVENTS and due(cursor[0]) <= time:
            pump(1)

    def pump_to(g, n=N_EVENTS):
        pump(max(0, g * N_EVENTS + n - cursor[0]))

    gain_copies = []
    for ry in range(ring):
        for rz in range(ring):
            if ry or rz:
                k = rz * ring + ry
                remote(gain_ref, gbuf.at[me], gsend.at[k], grecv.at[k], dev_data(ry, rz)).start()
                gain_copies.append((k, ry, rz))
    for copy in locals_:
        copy.wait()
    start_group(0)
    for k, ry, rz in gain_copies:
        src = gbuf.at[data_at(-ry, -rz)]
        remote(gain_ref, src, gsend.at[k], grecv.at[k], partner).wait()

    class Gather:
        def __init__(self, layer, kind, block):
            self.layer, self.kind, self.block, self.sent = layer, kind, block, []

        def send(self, idx, place, to):
            def build():
                ref = self.block(*place)
                dev = partner if to == 0 else dev_x(to)
                return remote(ref, ref, asend.at[self.layer, self.kind, idx], arecv.at[self.layer, self.kind, idx], dev)
            build().start()
            self.sent.append(build)

        def wait(self, idx, ref):
            remote(ref, ref, asend.at[self.layer, self.kind, idx], arecv.at[self.layer, self.kind, idx], partner).wait_recv()

        def start(self):
            self.send(0, (0, cc), 1)
            self.send(1, (0, cc), -1)
            self.send(4, (0, cc), 0)

        def near(self):
            self.wait(0, self.block(-1, cc))
            self.send(2, (-1, cc, 0), 1)
            self.send(5, (-1, cc), 0)
            self.wait(1, self.block(1, cc))
            self.send(3, (1, cc, 1), -1)
            self.send(6, (1, cc), 0)

        def far(self):
            self.wait(2, self.block(2, cc, 0))
            self.send(7, (2, cc, 0), 0)
            self.wait(3, self.block(2, cc, 1))
            self.send(8, (2, cc, 1), 0)

        def rest(self):
            block = self.block
            self.wait(4, block(0, 1 - cc))
            self.wait(5, block(-1, 1 - cc))
            self.wait(6, block(1, 1 - cc))
            self.wait(7, block(2, 1 - cc, 0))
            self.wait(8, block(2, 1 - cc, 1))

        def drain(self):
            for build in self.sent:
                build().wait_send()

    def h_block(rx, core, part=None):
        rows = pl.ds(pl.multiple_of((wrap(xx, rx) * 2 + core) * blk, 32), blk)
        return h_all.at[:, rows, :] if part is None else h_all.at[part, rows, :]

    def kv_block(rx, core, part=None):
        ref = kvx.at[wrap(xx, rx), core]
        return ref if part is None else ref.at[pl.ds(part * (seq // 2), seq // 2), :]

    def norm(layer):
        rows = pl.ds(pl.multiple_of(mi * blk, 32), blk)
        for b in range(batch):
            values = hid[b].astype(F32)
            centered = values - jnp.mean(values, axis=-1, keepdims=True)
            var = jnp.mean(centered * centered, axis=-1, keepdims=True)
            normed = centered * lax.rsqrt(var + EPS)
            for i in range(n_data):
                cols = slice(i * shard, (i + 1) * shard)
                h_all[b, rows, cols] = (normed[:, cols] * gbuf[i, layer:layer + 1, :]).astype(BF16)

    m_rows = seq // 2
    half_tiles = half_ff // head

    class Tile:
        def __init__(self, src, slot, pieces):
            self.copies = []
            at = 0
            for i, (start, n) in enumerate(pieces):
                self.copies.append(pltpu.make_async_copy(src.at[:, pl.ds(start, n)], wt.at[slot, :, pl.ds(at, n)], tsem.at[slot, i]))
                at += n

        def start(self):
            for copy in self.copies:
                copy.start()

        def wait(self):
            for copy in self.copies:
                copy.wait()

    def mlp_tile(layer, part, t, slot):
        src = (wi0 if part == 0 else wi1).at[layer]
        first = aligned((kvc + head if part == 0 else 0) + t * head, 128)
        return Tile(src, slot, ((first, head), (aligned(first + half_ff, 128), head)))

    def over_rows(fn):
        def body(i, carry):
            b = lax.div(i, 2)
            rows = pl.ds(pl.multiple_of(lax.rem(i, 2) * m_rows, m_rows), m_rows)
            fn(b, rows)
            return carry
        lax.fori_loop(0, 2 * batch, body, 0)

    def mlp(layer, part, begin, slot0, extra):
        blocks = 2 * batch

        def body(step, carry):
            t = lax.div(step, blocks)
            i = lax.rem(step, blocks)
            b = lax.div(i, 2)
            slot = lax.rem(t + slot0, 2)

            @pl.when(i == 0)
            def _():
                mlp_tile(layer, part, t, slot).wait()

            cols = pl.ds(pl.multiple_of(head + part * half_ff + t * head, head), head)
            for sub in range(m_rows // SUB):
                at = pl.ds(pl.multiple_of(lax.rem(i, 2) * m_rows + sub * SUB, SUB), SUB)
                res = dot(h_all[b, at, :], wt[slot])
                gate = res[:, :head].astype(BF16).astype(F32)
                up = res[:, head:].astype(BF16).astype(F32)
                joined[b, at, cols] = (gate * jax.nn.sigmoid(gate) * up).astype(BF16)

            @pl.when((i == blocks - 1) & (t + 2 < half_tiles))
            def _():
                mlp_tile(layer, part, t + 2, slot).start()

            for k in range(half_tiles * blocks):
                @pl.when(step == k)
                def _():
                    if k in extra:
                        extra[k]()
                    pump_until(begin + STEP * (k + 1))
            return carry

        lax.fori_loop(0, half_tiles * blocks, body, 0)

    def in_first(layer, kv, begin):
        kvq = Tile(wi0.at[layer], 0, ((0, kvc + head),))
        kvq.start()
        mlp_tile(layer, 0, 0, 1).start()
        kvq.wait()

        def do_kv(i, carry):
            rows = pl.ds(pl.multiple_of(i * m_rows, m_rows), m_rows)
            kvx[xx, cc, rows, :] = dot(h_all[cc, rows, :], wt[0, :, :kvc]).astype(BF16)
            return carry

        def do_q(b, rows):
            qb[b, rows, :] = dot(h_all[b, rows, :], wt[0, :, kvc:kvc + head]).astype(BF16)

        lax.fori_loop(0, 2, do_kv, 0)
        kv.start()
        pump_until(begin + 1)
        over_rows(do_q)
        mlp_tile(layer, 0, 1, 0).start()
        pump_until(begin + 3)

        mlp(layer, 0, begin + 3, 1, {5: kv.near, 9: kv.far})
        kv.rest()

    def in_second(layer, begin, then):
        mlp_tile(layer, 1, 0, 0).start()
        mlp_tile(layer, 1, 1, 1).start()
        mlp(layer, 1, begin, 0, {13: then})

    def wo_load(layer, k):
        return [pltpu.make_async_copy(woutb.at[layer, data_at(*BLOCKS[i])], wo.at[:, pl.ds(i * shard, shard)], osem.at[i])
                for i in range(*CHUNKS[k])]

    q_rows = 256

    def attention():
        def body(b, carry):
            for m in range(seq // q_rows):
                keys = (m + 1) * q_rows
                q = qb[b, m * q_rows:(m + 1) * q_rows, :]
                k = jnp.concatenate([kvx[0, b, :keys, :], kvx[1, b, :keys, :]], axis=-1)
                v = jnp.concatenate([kvx[2, b, :keys, :], kvx[3, b, :keys, :]], axis=-1)
                s = lax.dot_general(q, k, (((1,), (1,)), ((), ())), preferred_element_type=F32) * head ** -0.5
                row = lax.broadcasted_iota(jnp.int32, (q_rows, keys), 0) + m * q_rows
                col = lax.broadcasted_iota(jnp.int32, (q_rows, keys), 1)
                allowed = (col <= row) & (col < len_ref[b])
                s = jnp.where(allowed, s, NEG_BIG)
                e = jnp.exp(s - jnp.max(s, axis=-1, keepdims=True))
                p = e / jnp.sum(e, axis=-1, keepdims=True)
                o = dot(p, v.astype(F32))
                joined[b, m * q_rows:(m + 1) * q_rows, :head] = o.astype(BF16)
            return carry
        lax.fori_loop(0, batch, body, 0)

    PAIRS = (2, 1, -1, 0)
    pair_rows = 2 * blk

    def chunk_ds(k):
        first, last = CHUNKS[k]
        return pl.ds(first * shard, (last - first) * shard)

    def over_cols(k, fn):
        first, last = CHUNKS[k]

        def body(n, carry):
            fn(pl.ds(pl.multiple_of(first * shard + n * TILE, TILE), TILE))
            return carry
        lax.fori_loop(0, (last - first) * shard // TILE, body, 0)

    def out_proj(k, p):
        rows = pl.ds(pl.multiple_of(wrap(xx, PAIRS[p]) * pair_rows, 64), pair_rows)

        def fn(cols):
            lhs = joined[:, rows, :].reshape(batch * pair_rows, out_rows)
            res = dot(lhs, wo[:, cols]).astype(BF16)
            zp[p, :, :, cols] = res.reshape(batch, pair_rows, TILE)
        over_cols(k, fn)

    mine_rows = pl.ds(pl.multiple_of(cc * blk, 32), blk)
    other_rows = pl.ds(pl.multiple_of((1 - cc) * blk, 32), blk)

    class Scatter:
        def __init__(self, layer, k, out_ref):
            self.layer, self.k, self.out_ref, self.sent = layer, k, out_ref, []

        def send(self, idx, src, dst, dev):
            copy = remote(src, dst, rsend.at[self.layer, self.k, idx], rrecv.at[self.layer, self.k, idx], dev)
            copy.start()
            self.sent.append(copy)

        def wait(self, idx, dst):
            remote(dst, dst, rsend.at[self.layer, self.k, idx], rrecv.at[self.layer, self.k, idx], partner).wait_recv()

        def begin(self, p):
            here = chunk_ds(self.k)
            self.send(p, zp.at[p, :, other_rows, here], zrp.at[p, :, :, here], partner)

        def finish(self, p):
            k = self.k
            here = chunk_ds(k)

            def base(p, b, cols):
                return zp[p, b, mine_rows, cols].astype(F32) + zrp[p, b, :, cols].astype(F32)

            self.wait(p, zrp.at[p, :, :, here])
            if p == 0:
                def fn(cols):
                    for b in range(batch):
                        zs[0, b, :, cols] = base(0, b, cols).astype(BF16)
                over_cols(k, fn)
                self.send(4, zs.at[0, 0, :, here], xh.at[0, :, here], dev_x(1))
                self.send(5, zs.at[0, 1, :, here], xh.at[1, :, here], dev_x(-1))
            elif p < 3:
                self.wait(3 + p, xh.at[p - 1, :, here])

                def fn(cols):
                    for b in range(batch):
                        total = base(p, b, cols)
                        if b == p - 1:
                            total = total + xh[p - 1, :, cols].astype(F32)
                        zs[p, b, :, cols] = total.astype(BF16)
                over_cols(k, fn)
                self.send(5 + p, zs.at[p, :, :, here], xf.at[p - 1, :, :, here], dev_x(1 if p == 1 else -1))
            else:
                self.wait(6, xf.at[0, :, :, here])
                self.wait(7, xf.at[1, :, :, here])
                for b in range(batch):
                    for i in range(*CHUNKS[k]):
                        cols = slice(i * shard, (i + 1) * shard)
                        total = base(3, b, cols) + xf[0, b, :, cols].astype(F32) + xf[1, b, :, cols].astype(F32)
                        place = pl.ds(pl.multiple_of(data_at(*BLOCKS[i]) * shard, shard), shard)
                        self.out_ref[b, :, place] = (hid[b, :, place].astype(F32) + total).astype(BF16)

    for layer in (0, 1):
        g = 3 * layer
        h = Gather(layer, 0, h_block)
        norm(layer)
        h.start()
        near, far, first, second, chunk_times = PHASES[layer]
        pump_until(near)
        h.near()
        pump_until(far)
        h.far()
        h.rest()
        pump_to(g)
        kv = Gather(layer, 1, kv_block)
        in_first(layer, kv, first)
        attention()
        pump_to(g + 1)
        loads = [wo_load(layer, k) for k in range(len(CHUNKS))]

        def load(k):
            pump_to(g + 2, CHUNK_EVENTS[k])
            for copy in wo_load(layer, k):
                copy.start()

        in_second(layer, second, lambda: load(0))
        h.drain()
        kv.drain()
        parts = [Scatter(layer, k, hid if layer == 0 else y_ref) for k in range(len(CHUNKS))]
        for k, part in enumerate(parts):
            for copy in loads[k]:
                copy.wait()
            for p in range(4):
                out_proj(k, p)
                part.begin(p)
                if p == 2 and k + 1 < len(CHUNKS):
                    load(k + 1)
                else:
                    pump_until(chunk_times[k] + 2 * (p + 1))
                if p:
                    part.finish(p - 1)
                if p == 2 and k:
                    parts[k - 1].finish(3)
        parts[-1].finish(3)
        for part in parts:
            for copy in part.sent:
                copy.wait_send()

    for build in drains:
        build().wait_send()


def solution(mesh):
    batch_spec = ('replica', 'data')
    model_size = mesh.shape['model']
    n_data = mesh.shape['data']
    ring = 4
    assert model_size == 2 * ring and n_data == ring * ring

    def device_body(x_in, lengths, norm_gain, w_in, w_kv, w_out):
        batch, blk, width = x_in.shape
        layers, shard, in_cols = w_in.shape
        out_rows = w_out.shape[1]
        head = w_kv.shape[-1] // 2
        seq = blk * model_size
        ff = out_rows - head
        kvc = 2 * head // ring
        vmem = pl.BlockSpec(memory_space=pltpu.VMEM)
        hbm = pl.BlockSpec(memory_space=pl.ANY)
        dma = pltpu.SemaphoreType.DMA
        groups = len(GROUPS)
        y = pl.pallas_call(
            lambda *refs: layer_kernel(ring, *refs),
            name='layers',
            out_shape=(
                jax.ShapeDtypeStruct(x_in.shape, BF16),
                jax.ShapeDtypeStruct((layers, width, kvc + head + ff), BF16),
                jax.ShapeDtypeStruct((layers, width, ff), BF16),
                jax.ShapeDtypeStruct((layers, n_data, out_rows, shard), BF16),
            ),
            in_specs=[vmem, pl.BlockSpec(memory_space=pltpu.SMEM)] + [vmem] * 4,
            out_specs=(vmem, hbm, hbm, hbm),
            scratch_shapes=[
                pltpu.VMEM((8, shard), F32),
                pltpu.VMEM((batch, seq, width), BF16),
                pltpu.VMEM((batch, seq, out_rows), BF16),
                pltpu.VMEM((ring, batch, seq, kvc), BF16),
                pltpu.VMEM((batch, seq, head), BF16),
                pltpu.VMEM((2, width, TILE), BF16),
                pltpu.VMEM((out_rows, width), BF16),
                pltpu.VMEM((4, batch, 2 * blk, width), BF16),
                pltpu.VMEM((4, batch, blk, width), BF16),
                pltpu.VMEM((2, blk, width), BF16),
                pltpu.VMEM((2, batch, blk, width), BF16),
                pltpu.VMEM((3, batch, blk, width), BF16),
                pltpu.VMEM((batch, blk, width), BF16),
                pltpu.VMEM((n_data, 8, shard), F32),
                dma((n_data,)), dma((n_data,)),
                dma((groups, 2, 16)), dma((groups, 2, 16)),
                dma((2, 2, 9)), dma((2, 2, 9)),
                dma((2, 3, 8)), dma((2, 3, 8)),
                dma((2, 6)), dma((2, 2)), dma((n_data,)),
            ],
            compiler_params=pltpu.CompilerParams(
                collective_id=0, has_side_effects=True, vmem_limit_bytes=67043328),
            cost_estimate=pl.CostEstimate(flops=90_000_000_000, bytes_accessed=200_000_000, transcendentals=0),
        )(x_in, lengths, norm_gain, w_in, w_kv, w_out)[0]
        return y

    in_specs = (P(batch_spec, 'model', None), P(batch_spec), P(None, 'data'), P(None, 'data', 'model'), P(None, 'data', None), P(None, 'model', 'data'))
    return jax.shard_map(device_body, mesh=mesh, in_specs=in_specs, out_specs=P(batch_spec, 'model', None), check_vma=False)
```

```python
import jax
import jax.numpy as jnp
from jax import lax
from jax.experimental import pallas as pl
from jax.experimental.pallas import tpu as pltpu
from jax.sharding import PartitionSpec as P

EPS = 1e-6
NEG_BIG = -1e30
MESH = pl.DeviceIdType.MESH
TILE = 512
BOTH = (0, 1)
RELS = (0, -1, 1, 2)
KINDS = ('i0', 'i1', 'o')
GROUPS = tuple((layer, kind) for layer in BOTH for kind in KINDS)
F32 = jnp.float32
BF16 = jnp.bfloat16
ORDER = ((0, 1), (4, 8), (2, 3), (5, 9), (6, 10), (7, 11), (12, 13), (14, 15))
N_EVENTS = 32
START_NEXT = 14
EARLY = 8
SHIFT = 10
OFFSETS = (0, 1.5, 7.5, 13.5, 19.5, 32, 38, 47)
BEGINS = (15, 72, 117, 165, 215, 259)
PHASES = ((34, 43, 74, 118, (140, 168, 174)), (203, 211, 217, 261, (283, 294, 304)))
STEP = 1.5
SUB = 128
BLOCKS = ((0, 0), (1, 0), (-1, 0), (0, 1), (0, -1), (1, 1), (-1, -1), (1, -1),
          (-1, 1), (2, 0), (0, 2), (2, -1), (-1, 2), (1, 2), (2, 1), (2, 2))
CHUNKS = ((0, 8), (8, 12), (12, 16))
CHUNK_EVENTS = (20, 28, 32)


def aligned(value, n):
    return value if isinstance(value, int) else pl.multiple_of(value, n)


def dot(a, b):
    return jnp.dot(a, b, preferred_element_type=F32)


def layer_kernel(ring, x_ref, len_ref, gain_in, win_ref, wkv_ref, wout_ref, y_ref, wi0, wi1, woutb,
                 gain_ref, h_all, joined, kvx, qb, wt, wo, zp, zrp, xh, xf, zs, hid, gbuf,
                 gsend, grecv, wsend, wrecv, asend, arecv, rsend, rrecv, bsem, tsem, osem):
    batch, blk, width = x_ref.shape
    shard = win_ref.shape[1]
    out_rows = wout_ref.shape[1]
    head = qb.shape[-1]
    kvc = kvx.shape[-1]
    seq = h_all.shape[1]
    n_data = gbuf.shape[0]
    ff = out_rows - head
    half_ff = ff // 2
    me = lax.axis_index('data')
    mi = lax.axis_index('model')
    yy = lax.rem(me, ring)
    zz = lax.div(me, ring)
    xx = lax.div(mi, 2)
    cc = lax.rem(mi, 2)

    def wrap(value, rel):
        return lax.rem(value + (rel + ring), ring)

    def data_at(ry, rz):
        return wrap(zz, rz) * ring + wrap(yy, ry)

    def dev_data(ry, rz):
        return {'data': data_at(ry, rz), 'model': mi}

    def dev_x(rx):
        return {'data': me, 'model': wrap(xx, rx) * 2 + cc}

    partner = {'data': me, 'model': xx * 2 + (1 - cc)}

    barrier = pltpu.get_barrier_semaphore()
    for ry in range(ring):
        for rz in range(ring):
            if ry or rz:
                pl.semaphore_signal(barrier, inc=1, device_id=dev_data(ry, rz), device_id_type=MESH)
    for dev in (dev_x(1), dev_x(-1), partner):
        pl.semaphore_signal(barrier, inc=1, device_id=dev, device_id_type=MESH)

    my_rows = pl.ds(pl.multiple_of(me * shard, 128), shard)
    locals_ = []

    def local(layer, i, src, dst):
        locals_.append(pltpu.make_async_copy(src, dst, bsem.at[layer, i]))

    for layer in BOTH:
        kv_cols = pl.ds(pl.multiple_of(xx * kvc, 128), kvc)
        local(layer, 0, wkv_ref.at[layer, :, kv_cols], wi0.at[layer, my_rows, pl.ds(0, kvc)])
        local(layer, 1, win_ref.at[layer, :, pl.ds(0, head + half_ff)], wi0.at[layer, my_rows, pl.ds(kvc, head + half_ff)])
        local(layer, 2, win_ref.at[layer, :, pl.ds(head + ff, half_ff)], wi0.at[layer, my_rows, pl.ds(kvc + head + half_ff, half_ff)])
        local(layer, 3, win_ref.at[layer, :, pl.ds(head + half_ff, half_ff)], wi1.at[layer, my_rows, pl.ds(0, half_ff)])
        local(layer, 4, win_ref.at[layer, :, pl.ds(head + ff + half_ff, half_ff)], wi1.at[layer, my_rows, pl.ds(half_ff, half_ff)])
        local(layer, 5, wout_ref.at[layer], woutb.at[layer, me])
    for copy in locals_:
        copy.start()
    gain_ref[0:gain_in.shape[0], :] = gain_in[...].astype(F32)
    gbuf[me] = gain_ref[...]
    hid[...] = x_ref[...]
    pl.semaphore_wait(barrier, n_data - 1 + 3)

    drains = []

    def remote(src, dst, ssem, rsem, dev):
        return pltpu.make_async_remote_copy(src_ref=src, dst_ref=dst, send_sem=ssem, recv_sem=rsem,
                                            device_id=dev, device_id_type=MESH)

    half_in = shard // 2
    half_out = out_rows // 2

    def unit(g, hf, rp, rq, part=None):
        layer, kind = GROUPS[g]
        s = data_at(rp, rq) if hf == 0 else data_at(rq, rp)
        if kind == 'o':
            n = half_out if part is None else half_out // 2
            return woutb.at[layer, s, pl.ds(hf * half_out + (0 if part is None else part * n), n), :]
        n = half_in if part is None else half_in // 2
        start = pl.multiple_of(s * shard + (hf * half_in + (0 if part is None else part * n)), 32)
        return (wi0 if kind == 'i0' else wi1).at[layer, pl.ds(start, n), :]

    def along(hf, primary, rel):
        on_y = (hf == 0) == primary
        return dev_data(rel, 0) if on_y else dev_data(0, rel)

    def send(g, hf, idx, rel, primary, to, part=None):
        def build():
            ref = unit(g, hf, rel[0], rel[1], part)
            return remote(ref, ref, wsend.at[g, hf, idx], wrecv.at[g, hf, idx], along(hf, primary, to))
        build().start()
        drains.append(build)

    def spec(idx):
        if idx < 4:
            return ((-1, 0, None), (1, 0, None), (2, 0, 0), (2, 0, 1))[idx]
        return (RELS[idx % 4], (None, -1, 1, 2)[idx // 4], None)

    def start_group(g):
        for hf in BOTH:
            send(g, hf, 0, (0, 0), True, 1)
            send(g, hf, 1, (0, 0), True, -1)
        for hf in BOTH:
            send(g, hf, 4, (0, 0), False, 1)
            send(g, hf, 8, (0, 0), False, -1)

    def arrive(g, hf, idx):
        rp, rq, part = spec(idx)
        ref = unit(g, hf, rp, rq, part)
        remote(ref, ref, wsend.at[g, hf, idx], wrecv.at[g, hf, idx], along(hf, True, 1)).wait_recv()
        if idx < 2:
            send(g, hf, idx + 2, (rp, rq), True, -rp, idx)
        elif idx == 3:
            send(g, hf, 7, (rp, rq), False, 1)
            send(g, hf, 11, (rp, rq), False, -1)
        elif idx in (4, 5):
            send(g, hf, idx + 8, (rp, rq), False, 1)
        elif idx in (10, 11):
            send(g, hf, idx + 4, (rp, rq), False, -1)

    def turn_neighbors(g):
        for hf in BOTH:
            for at in (1, 2):
                send(g, hf, at + 4, (RELS[at], 0), False, 1)
                send(g, hf, at + 8, (RELS[at], 0), False, -1)

    sequence = [(hf, idx) for pair in ORDER for hf in BOTH for idx in pair]
    order = sorted(((g, k) for g in range(len(GROUPS)) for k in range(N_EVENTS)),
                   key=lambda e: e[0] * N_EVENTS + e[1] - (SHIFT if e[1] < EARLY and e[0] else 0))
    cursor = [0]

    def pump(n):
        for _ in range(n):
            g, k = order[cursor[0]]
            if k == START_NEXT and g + 1 < len(GROUPS):
                start_group(g + 1)
            arrive(g, *sequence[k])
            if k == 3:
                turn_neighbors(g)
            cursor[0] += 1

    def pump_until(time):
        while cursor[0] < len(order):
            g, k = divmod(cursor[0], N_EVENTS)
            if BEGINS[g] + OFFSETS[k // 4] > time:
                break
            pump(1)

    def pump_to(g, n=N_EVENTS):
        pump(max(0, order.index((g, n - 1)) + 1 - cursor[0]))

    gain_copies = []
    for ry in range(ring):
        for rz in range(ring):
            if ry or rz:
                k = rz * ring + ry
                remote(gain_ref, gbuf.at[me], gsend.at[k], grecv.at[k], dev_data(ry, rz)).start()
                gain_copies.append((k, ry, rz))
    for copy in locals_:
        copy.wait()
    start_group(0)
    for k, ry, rz in gain_copies:
        src = gbuf.at[data_at(-ry, -rz)]
        remote(gain_ref, src, gsend.at[k], grecv.at[k], partner).wait()

    class Gather:
        def __init__(self, layer, kind, block):
            self.layer, self.kind, self.block, self.sent = layer, kind, block, []

        def send(self, idx, place, to):
            def build():
                ref = self.block(*place)
                dev = partner if to == 0 else dev_x(to)
                return remote(ref, ref, asend.at[self.layer, self.kind, idx], arecv.at[self.layer, self.kind, idx], dev)
            build().start()
            self.sent.append(build)

        def wait(self, idx, ref):
            remote(ref, ref, asend.at[self.layer, self.kind, idx], arecv.at[self.layer, self.kind, idx], partner).wait_recv()

        def start(self):
            self.send(0, (0, cc), 1)
            self.send(1, (0, cc), -1)
            self.send(4, (0, cc), 0)

        def near(self):
            self.wait(0, self.block(-1, cc))
            self.send(2, (-1, cc, 0), 1)
            self.send(5, (-1, cc), 0)
            self.wait(1, self.block(1, cc))
            self.send(3, (1, cc, 1), -1)
            self.send(6, (1, cc), 0)

        def far(self):
            self.wait(2, self.block(2, cc, 0))
            self.send(7, (2, cc, 0), 0)
            self.wait(3, self.block(2, cc, 1))
            self.send(8, (2, cc, 1), 0)

        def rest(self):
            block = self.block
            self.wait(4, block(0, 1 - cc))
            self.wait(5, block(-1, 1 - cc))
            self.wait(6, block(1, 1 - cc))
            self.wait(7, block(2, 1 - cc, 0))
            self.wait(8, block(2, 1 - cc, 1))

        def drain(self):
            for build in self.sent:
                build().wait_send()

    def h_block(rx, core, part=None):
        rows = pl.ds(pl.multiple_of((wrap(xx, rx) * 2 + core) * blk, 32), blk)
        return h_all.at[:, rows, :] if part is None else h_all.at[part, rows, :]

    def kv_block(rx, core, part=None):
        ref = kvx.at[wrap(xx, rx), core]
        return ref if part is None else ref.at[pl.ds(part * (seq // 2), seq // 2), :]

    def norm(layer):
        rows = pl.ds(pl.multiple_of(mi * blk, 32), blk)
        for b in range(batch):
            values = hid[b].astype(F32)
            centered = values - jnp.mean(values, axis=-1, keepdims=True)
            var = jnp.mean(centered * centered, axis=-1, keepdims=True)
            normed = centered * lax.rsqrt(var + EPS)
            for i in range(n_data):
                cols = slice(i * shard, (i + 1) * shard)
                h_all[b, rows, cols] = (normed[:, cols] * gbuf[i, layer:layer + 1, :]).astype(BF16)

    m_rows = seq // 2
    half_tiles = half_ff // head

    class Tile:
        def __init__(self, src, slot, pieces):
            self.copies = []
            at = 0
            for i, (start, n) in enumerate(pieces):
                self.copies.append(pltpu.make_async_copy(src.at[:, pl.ds(start, n)], wt.at[slot, :, pl.ds(at, n)], tsem.at[slot, i]))
                at += n

        def start(self):
            for copy in self.copies:
                copy.start()

        def wait(self):
            for copy in self.copies:
                copy.wait()

    def mlp_tile(layer, part, t, slot):
        src = (wi0 if part == 0 else wi1).at[layer]
        first = aligned((kvc + head if part == 0 else 0) + t * head, 128)
        return Tile(src, slot, ((first, head), (aligned(first + half_ff, 128), head)))

    def over_rows(fn):
        def body(i, carry):
            b = lax.div(i, 2)
            rows = pl.ds(pl.multiple_of(lax.rem(i, 2) * m_rows, m_rows), m_rows)
            fn(b, rows)
            return carry
        lax.fori_loop(0, 2 * batch, body, 0)

    def mlp(layer, part, begin, slot0, extra):
        blocks = 2 * batch

        def body(step, carry):
            t = lax.div(step, blocks)
            i = lax.rem(step, blocks)
            b = lax.div(i, 2)
            slot = lax.rem(t + slot0, 2)

            @pl.when(i == 0)
            def _():
                mlp_tile(layer, part, t, slot).wait()

            cols = pl.ds(pl.multiple_of(head + part * half_ff + t * head, head), head)
            for sub in range(m_rows // SUB):
                at = pl.ds(pl.multiple_of(lax.rem(i, 2) * m_rows + sub * SUB, SUB), SUB)
                res = dot(h_all[b, at, :], wt[slot])
                gate = res[:, :head].astype(BF16).astype(F32)
                up = res[:, head:].astype(BF16).astype(F32)
                joined[b, at, cols] = (gate * jax.nn.sigmoid(gate) * up).astype(BF16)

            @pl.when((i == blocks - 1) & (t + 2 < half_tiles))
            def _():
                mlp_tile(layer, part, t + 2, slot).start()

            for k in range(half_tiles * blocks):
                @pl.when(step == k)
                def _():
                    if k in extra:
                        extra[k]()
                    pump_until(begin + STEP * (k + 1))
            return carry

        lax.fori_loop(0, half_tiles * blocks, body, 0)

    def in_first(layer, kv, begin):
        kvq = Tile(wi0.at[layer], 0, ((0, kvc + head),))
        kvq.start()
        mlp_tile(layer, 0, 0, 1).start()
        kvq.wait()

        def do_kv(i, carry):
            rows = pl.ds(pl.multiple_of(i * m_rows, m_rows), m_rows)
            kvx[xx, cc, rows, :] = dot(h_all[cc, rows, :], wt[0, :, :kvc]).astype(BF16)
            return carry

        def do_q(b, rows):
            qb[b, rows, :] = dot(h_all[b, rows, :], wt[0, :, kvc:kvc + head]).astype(BF16)

        lax.fori_loop(0, 2, do_kv, 0)
        kv.start()
        pump_until(begin + 1)
        over_rows(do_q)
        mlp_tile(layer, 0, 1, 0).start()
        pump_until(begin + 3)

        mlp(layer, 0, begin + 3, 1, {5: kv.near, 9: kv.far})
        kv.rest()

    def in_second(layer, begin, then):
        mlp_tile(layer, 1, 0, 0).start()
        mlp_tile(layer, 1, 1, 1).start()
        mlp(layer, 1, begin, 0, {13: then})

    def wo_load(layer, k):
        return [pltpu.make_async_copy(woutb.at[layer, data_at(*BLOCKS[i])], wo.at[:, pl.ds(i * shard, shard)], osem.at[i])
                for i in range(*CHUNKS[k])]

    q_rows = 256

    def attention():
        def body(b, carry):
            for m in range(seq // q_rows):
                keys = (m + 1) * q_rows
                q = qb[b, m * q_rows:(m + 1) * q_rows, :]
                k = jnp.concatenate([kvx[0, b, :keys, :], kvx[1, b, :keys, :]], axis=-1)
                v = jnp.concatenate([kvx[2, b, :keys, :], kvx[3, b, :keys, :]], axis=-1)
                s = lax.dot_general(q, k, (((1,), (1,)), ((), ())), preferred_element_type=F32) * head ** -0.5
                row = lax.broadcasted_iota(jnp.int32, (q_rows, keys), 0) + m * q_rows
                col = lax.broadcasted_iota(jnp.int32, (q_rows, keys), 1)
                allowed = (col <= row) & (col < len_ref[b])
                s = jnp.where(allowed, s, NEG_BIG)
                e = jnp.exp(s - jnp.max(s, axis=-1, keepdims=True))
                p = e / jnp.sum(e, axis=-1, keepdims=True)
                o = dot(p, v.astype(F32))
                joined[b, m * q_rows:(m + 1) * q_rows, :head] = o.astype(BF16)
            return carry
        lax.fori_loop(0, batch, body, 0)

    PAIRS = (2, 1, -1, 0)
    pair_rows = 2 * blk

    def chunk_ds(k):
        first, last = CHUNKS[k]
        return pl.ds(first * shard, (last - first) * shard)

    def over_cols(k, fn):
        first, last = CHUNKS[k]

        def body(n, carry):
            fn(pl.ds(pl.multiple_of(first * shard + n * TILE, TILE), TILE))
            return carry
        lax.fori_loop(0, (last - first) * shard // TILE, body, 0)

    def out_proj(k, p):
        rows = pl.ds(pl.multiple_of(wrap(xx, PAIRS[p]) * pair_rows, 64), pair_rows)

        def fn(cols):
            lhs = joined[:, rows, :].reshape(batch * pair_rows, out_rows)
            res = dot(lhs, wo[:, cols]).astype(BF16)
            zp[p, :, :, cols] = res.reshape(batch, pair_rows, TILE)
        over_cols(k, fn)

    mine_rows = pl.ds(pl.multiple_of(cc * blk, 32), blk)
    other_rows = pl.ds(pl.multiple_of((1 - cc) * blk, 32), blk)

    class Scatter:
        def __init__(self, layer, k, out_ref):
            self.layer, self.k, self.out_ref, self.sent = layer, k, out_ref, []

        def send(self, idx, src, dst, dev):
            copy = remote(src, dst, rsend.at[self.layer, self.k, idx], rrecv.at[self.layer, self.k, idx], dev)
            copy.start()
            self.sent.append(copy)

        def wait(self, idx, dst):
            remote(dst, dst, rsend.at[self.layer, self.k, idx], rrecv.at[self.layer, self.k, idx], partner).wait_recv()

        def begin(self, p):
            here = chunk_ds(self.k)
            self.send(p, zp.at[p, :, other_rows, here], zrp.at[p, :, :, here], partner)

        def finish(self, p):
            k = self.k
            here = chunk_ds(k)

            def base(p, b, cols):
                return zp[p, b, mine_rows, cols].astype(F32) + zrp[p, b, :, cols].astype(F32)

            self.wait(p, zrp.at[p, :, :, here])
            if p == 0:
                def fn(cols):
                    for b in range(batch):
                        zs[0, b, :, cols] = base(0, b, cols).astype(BF16)
                over_cols(k, fn)
                self.send(4, zs.at[0, 0, :, here], xh.at[0, :, here], dev_x(1))
                self.send(5, zs.at[0, 1, :, here], xh.at[1, :, here], dev_x(-1))
            elif p < 3:
                self.wait(3 + p, xh.at[p - 1, :, here])

                def fn(cols):
                    for b in range(batch):
                        total = base(p, b, cols)
                        if b == p - 1:
                            total = total + xh[p - 1, :, cols].astype(F32)
                        zs[p, b, :, cols] = total.astype(BF16)
                over_cols(k, fn)
                self.send(5 + p, zs.at[p, :, :, here], xf.at[p - 1, :, :, here], dev_x(1 if p == 1 else -1))
            else:
                self.wait(6, xf.at[0, :, :, here])
                self.wait(7, xf.at[1, :, :, here])
                for b in range(batch):
                    for i in range(*CHUNKS[k]):
                        cols = slice(i * shard, (i + 1) * shard)
                        total = base(3, b, cols) + xf[0, b, :, cols].astype(F32) + xf[1, b, :, cols].astype(F32)
                        place = pl.ds(pl.multiple_of(data_at(*BLOCKS[i]) * shard, shard), shard)
                        self.out_ref[b, :, place] = (hid[b, :, place].astype(F32) + total).astype(BF16)

    for layer in BOTH:
        g = 3 * layer
        h = Gather(layer, 0, h_block)
        norm(layer)
        h.start()
        near, far, first, second, chunk_times = PHASES[layer]
        pump_until(near)
        h.near()
        pump_until(far)
        h.far()
        h.rest()
        pump_to(g)
        kv = Gather(layer, 1, kv_block)
        in_first(layer, kv, first)
        attention()
        pump_to(g + 1)
        loads = [wo_load(layer, k) for k in range(len(CHUNKS))]

        def load(k):
            pump_to(g + 2, CHUNK_EVENTS[k])
            for copy in wo_load(layer, k):
                copy.start()

        in_second(layer, second, lambda: load(0))
        h.drain()
        kv.drain()
        parts = [Scatter(layer, k, hid if layer == 0 else y_ref) for k in range(len(CHUNKS))]
        for k, part in enumerate(parts):
            for copy in loads[k]:
                copy.wait()
            for p in range(4):
                out_proj(k, p)
                part.begin(p)
                pump_until(chunk_times[k] + p)
                if p:
                    part.finish(p - 1)
                if p == 2 and k:
                    parts[k - 1].finish(3)
            if part is not parts[-1]:
                load(k + 1)
            else:
                pump_until(chunk_times[k] + 6)
        parts[-1].finish(3)
        for part in parts:
            for copy in part.sent:
                copy.wait_send()

    for build in drains:
        build().wait_send()


def solution(mesh):
    batch_spec = ('replica', 'data')
    model_size = mesh.shape['model']
    n_data = mesh.shape['data']
    ring = 4
    assert model_size == 2 * ring and n_data == ring * ring

    def device_body(x_in, lengths, norm_gain, w_in, w_kv, w_out):
        batch, blk, width = x_in.shape
        layers, shard, in_cols = w_in.shape
        out_rows = w_out.shape[1]
        head = w_kv.shape[-1] // 2
        seq = blk * model_size
        ff = out_rows - head
        kvc = 2 * head // ring
        vmem = pl.BlockSpec(memory_space=pltpu.VMEM)
        hbm = pl.BlockSpec(memory_space=pl.ANY)
        dma = pltpu.SemaphoreType.DMA
        groups = len(GROUPS)
        y = pl.pallas_call(
            lambda *refs: layer_kernel(ring, *refs),
            name='layers',
            out_shape=(
                jax.ShapeDtypeStruct(x_in.shape, BF16),
                jax.ShapeDtypeStruct((layers, width, kvc + head + ff), BF16),
                jax.ShapeDtypeStruct((layers, width, ff), BF16),
                jax.ShapeDtypeStruct((layers, n_data, out_rows, shard), BF16),
            ),
            in_specs=[vmem, pl.BlockSpec(memory_space=pltpu.SMEM)] + [vmem] * 4,
            out_specs=(vmem, hbm, hbm, hbm),
            scratch_shapes=[
                pltpu.VMEM((8, shard), F32),
                pltpu.VMEM((batch, seq, width), BF16),
                pltpu.VMEM((batch, seq, out_rows), BF16),
                pltpu.VMEM((ring, batch, seq, kvc), BF16),
                pltpu.VMEM((batch, seq, head), BF16),
                pltpu.VMEM((2, width, TILE), BF16),
                pltpu.VMEM((out_rows, width), BF16),
                pltpu.VMEM((4, batch, 2 * blk, width), BF16),
                pltpu.VMEM((4, batch, blk, width), BF16),
                pltpu.VMEM((2, blk, width), BF16),
                pltpu.VMEM((2, batch, blk, width), BF16),
                pltpu.VMEM((3, batch, blk, width), BF16),
                pltpu.VMEM((batch, blk, width), BF16),
                pltpu.VMEM((n_data, 8, shard), F32),
                dma((n_data,)), dma((n_data,)),
                dma((groups, 2, 16)), dma((groups, 2, 16)),
                dma((2, 2, 9)), dma((2, 2, 9)),
                dma((2, 3, 8)), dma((2, 3, 8)),
                dma((2, 6)), dma((2, 2)), dma((n_data,)),
            ],
            compiler_params=pltpu.CompilerParams(
                collective_id=0, has_side_effects=True, vmem_limit_bytes=67043328),
            cost_estimate=pl.CostEstimate(flops=90_000_000_000, bytes_accessed=200_000_000, transcendentals=0),
        )(x_in, lengths, norm_gain, w_in, w_kv, w_out)[0]
        return y

    in_specs = (P(batch_spec, 'model', None), P(batch_spec), P(None, 'data'), P(None, 'data', 'model'), P(None, 'data', None), P(None, 'model', 'data'))
    return jax.shard_map(device_body, mesh=mesh, in_specs=in_specs, out_specs=P(batch_spec, 'model', None), check_vma=False)
```

```python
import jax
import jax.numpy as jnp
from jax import lax
from jax.experimental import pallas as pl
from jax.experimental.pallas import tpu as pltpu
from jax.sharding import PartitionSpec as P

EPS = 1e-6
NEG_BIG = -1e30
MESH = pl.DeviceIdType.MESH
TILE = 512
BOTH = (0, 1)
RELS = (0, -1, 1, 2)
KINDS = ('i0', 'i1', 'o')
GROUPS = tuple((layer, kind) for layer in BOTH for kind in KINDS)
F32 = jnp.float32
BF16 = jnp.bfloat16
ORDER = ((0, 1), (4, 8), (2, 3), (5, 9), (6, 10), (7, 11), (12, 13), (14, 15))
N_EVENTS = 32
START_NEXT = 14
EARLY = 8
SHIFT = 10
OFFSETS = (0, 1.5, 7.5, 13.5, 19.5, 32, 38, 47)
BEGINS = (15, 72, 117, 165, 215, 259)
PHASES = ((34, 43, 74, 118, (140, 168, 174)), (204, 216, 219, 261, (283, 294, 304)))
STEP = 1.5
LAGS = (2, 5, 5, 8)
SUB = 128
BLOCKS = ((0, 0), (1, 0), (-1, 0), (0, 1), (0, -1), (1, 1), (-1, -1), (1, -1),
          (-1, 1), (2, 0), (0, 2), (2, -1), (-1, 2), (1, 2), (2, 1), (2, 2))
CHUNKS = ((0, 8), (8, 12), (12, 16))
CHUNK_EVENTS = (20, 28, 32)


def aligned(value, n):
    return value if isinstance(value, int) else pl.multiple_of(value, n)


def dot(a, b):
    return jnp.dot(a, b, preferred_element_type=F32)


def layer_kernel(ring, x_ref, len_ref, gain_in, win_ref, wkv_ref, wout_ref, y_ref, wi0, wi1, woutb,
                 gain_ref, h_all, joined, kvx, qb, wt, wo, zp, zrp, xh, xf, zs, hid, gbuf,
                 gsend, grecv, wsend, wrecv, asend, arecv, rsend, rrecv, bsem, tsem, osem):
    batch, blk, width = x_ref.shape
    shard = win_ref.shape[1]
    out_rows = wout_ref.shape[1]
    head = qb.shape[-1]
    kvc = kvx.shape[-1]
    seq = h_all.shape[1]
    n_data = gbuf.shape[0]
    ff = out_rows - head
    half_ff = ff // 2
    me = lax.axis_index('data')
    mi = lax.axis_index('model')
    yy = lax.rem(me, ring)
    zz = lax.div(me, ring)
    xx = lax.div(mi, 2)
    cc = lax.rem(mi, 2)

    def wrap(value, rel):
        return lax.rem(value + (rel + ring), ring)

    def data_at(ry, rz):
        return wrap(zz, rz) * ring + wrap(yy, ry)

    def dev_data(ry, rz):
        return {'data': data_at(ry, rz), 'model': mi}

    def dev_x(rx):
        return {'data': me, 'model': wrap(xx, rx) * 2 + cc}

    partner = {'data': me, 'model': xx * 2 + (1 - cc)}

    barrier = pltpu.get_barrier_semaphore()
    for ry in range(ring):
        for rz in range(ring):
            if ry or rz:
                pl.semaphore_signal(barrier, inc=1, device_id=dev_data(ry, rz), device_id_type=MESH)
    for dev in (dev_x(1), dev_x(-1), partner):
        pl.semaphore_signal(barrier, inc=1, device_id=dev, device_id_type=MESH)

    my_rows = pl.ds(pl.multiple_of(me * shard, 128), shard)
    locals_ = []

    def local(layer, i, src, dst):
        locals_.append(pltpu.make_async_copy(src, dst, bsem.at[layer, i]))

    for layer in BOTH:
        kv_cols = pl.ds(pl.multiple_of(xx * kvc, 128), kvc)
        local(layer, 0, wkv_ref.at[layer, :, kv_cols], wi0.at[layer, my_rows, pl.ds(0, kvc)])
        local(layer, 1, win_ref.at[layer, :, pl.ds(0, head + half_ff)], wi0.at[layer, my_rows, pl.ds(kvc, head + half_ff)])
        local(layer, 2, win_ref.at[layer, :, pl.ds(head + ff, half_ff)], wi0.at[layer, my_rows, pl.ds(kvc + head + half_ff, half_ff)])
        local(layer, 3, win_ref.at[layer, :, pl.ds(head + half_ff, half_ff)], wi1.at[layer, my_rows, pl.ds(0, half_ff)])
        local(layer, 4, win_ref.at[layer, :, pl.ds(head + ff + half_ff, half_ff)], wi1.at[layer, my_rows, pl.ds(half_ff, half_ff)])
        local(layer, 5, wout_ref.at[layer], woutb.at[layer, me])
    for copy in locals_:
        copy.start()
    gain_ref[0:gain_in.shape[0], :] = gain_in[...].astype(F32)
    gbuf[me] = gain_ref[...]
    hid[...] = x_ref[...]
    pl.semaphore_wait(barrier, n_data - 1 + 3)

    drains = []

    def remote(src, dst, ssem, rsem, dev):
        return pltpu.make_async_remote_copy(src_ref=src, dst_ref=dst, send_sem=ssem, recv_sem=rsem,
                                            device_id=dev, device_id_type=MESH)

    half_in = shard // 2
    half_out = out_rows // 2

    def unit(g, hf, rp, rq, part=None):
        layer, kind = GROUPS[g]
        s = data_at(rp, rq) if hf == 0 else data_at(rq, rp)
        if kind == 'o':
            n = half_out if part is None else half_out // 2
            return woutb.at[layer, s, pl.ds(hf * half_out + (0 if part is None else part * n), n), :]
        n = half_in if part is None else half_in // 2
        start = pl.multiple_of(s * shard + (hf * half_in + (0 if part is None else part * n)), 32)
        return (wi0 if kind == 'i0' else wi1).at[layer, pl.ds(start, n), :]

    def along(hf, primary, rel):
        on_y = (hf == 0) == primary
        return dev_data(rel, 0) if on_y else dev_data(0, rel)

    def send(g, hf, idx, rel, primary, to, part=None):
        def build():
            ref = unit(g, hf, rel[0], rel[1], part)
            return remote(ref, ref, wsend.at[g, hf, idx], wrecv.at[g, hf, idx], along(hf, primary, to))
        build().start()
        drains.append(build)

    def spec(idx):
        if idx < 4:
            return ((-1, 0, None), (1, 0, None), (2, 0, 0), (2, 0, 1))[idx]
        return (RELS[idx % 4], (None, -1, 1, 2)[idx // 4], None)

    def start_group(g):
        for hf in BOTH:
            send(g, hf, 0, (0, 0), True, 1)
            send(g, hf, 1, (0, 0), True, -1)
        for hf in BOTH:
            send(g, hf, 4, (0, 0), False, 1)
            send(g, hf, 8, (0, 0), False, -1)

    def arrive(g, hf, idx):
        rp, rq, part = spec(idx)
        ref = unit(g, hf, rp, rq, part)
        remote(ref, ref, wsend.at[g, hf, idx], wrecv.at[g, hf, idx], along(hf, True, 1)).wait_recv()
        if idx < 2:
            send(g, hf, idx + 2, (rp, rq), True, -rp, idx)
        elif idx == 3:
            send(g, hf, 7, (rp, rq), False, 1)
            send(g, hf, 11, (rp, rq), False, -1)
        elif idx in (4, 5):
            send(g, hf, idx + 8, (rp, rq), False, 1)
        elif idx in (10, 11):
            send(g, hf, idx + 4, (rp, rq), False, -1)

    def turn_neighbors(g):
        for hf in BOTH:
            for at in (1, 2):
                send(g, hf, at + 4, (RELS[at], 0), False, 1)
                send(g, hf, at + 8, (RELS[at], 0), False, -1)

    sequence = [(hf, idx) for pair in ORDER for hf in BOTH for idx in pair]
    order = sorted(((g, k) for g in range(len(GROUPS)) for k in range(N_EVENTS)),
                   key=lambda e: e[0] * N_EVENTS + e[1] - (SHIFT if e[1] < EARLY and e[0] else 0))
    cursor = [0]

    def pump(n):
        for _ in range(n):
            g, k = order[cursor[0]]
            if k == START_NEXT and g + 1 < len(GROUPS):
                start_group(g + 1)
            arrive(g, *sequence[k])
            if k == 3:
                turn_neighbors(g)
            cursor[0] += 1

    def pump_until(time):
        while cursor[0] < len(order):
            g, k = divmod(cursor[0], N_EVENTS)
            if BEGINS[g] + OFFSETS[k // 4] > time:
                break
            pump(1)

    def pump_to(g, n=N_EVENTS):
        pump(max(0, order.index((g, n - 1)) + 1 - cursor[0]))

    gain_copies = []
    for ry in range(ring):
        for rz in range(ring):
            if ry or rz:
                k = rz * ring + ry
                remote(gain_ref, gbuf.at[me], gsend.at[k], grecv.at[k], dev_data(ry, rz)).start()
                gain_copies.append((k, ry, rz))
    for copy in locals_:
        copy.wait()
    start_group(0)
    for k, ry, rz in gain_copies:
        src = gbuf.at[data_at(-ry, -rz)]
        remote(gain_ref, src, gsend.at[k], grecv.at[k], partner).wait()

    class Gather:
        def __init__(self, layer, kind, block):
            self.layer, self.kind, self.block, self.sent = layer, kind, block, []

        def send(self, idx, place, to):
            def build():
                ref = self.block(*place)
                dev = partner if to == 0 else dev_x(to)
                return remote(ref, ref, asend.at[self.layer, self.kind, idx], arecv.at[self.layer, self.kind, idx], dev)
            build().start()
            self.sent.append(build)

        def wait(self, idx, ref):
            remote(ref, ref, asend.at[self.layer, self.kind, idx], arecv.at[self.layer, self.kind, idx], partner).wait_recv()

        def start(self):
            self.send(0, (0, cc), 1)
            self.send(1, (0, cc), -1)
            self.send(4, (0, cc), 0)

        def near(self):
            self.wait(0, self.block(-1, cc))
            self.send(2, (-1, cc, 0), 1)
            self.send(5, (-1, cc), 0)
            self.wait(1, self.block(1, cc))
            self.send(3, (1, cc, 1), -1)
            self.send(6, (1, cc), 0)

        def far(self):
            self.wait(2, self.block(2, cc, 0))
            self.send(7, (2, cc, 0), 0)
            self.wait(3, self.block(2, cc, 1))
            self.send(8, (2, cc, 1), 0)

        def rest(self):
            block = self.block
            self.wait(4, block(0, 1 - cc))
            self.wait(5, block(-1, 1 - cc))
            self.wait(6, block(1, 1 - cc))
            self.wait(7, block(2, 1 - cc, 0))
            self.wait(8, block(2, 1 - cc, 1))

        def drain(self):
            for build in self.sent:
                build().wait_send()

    def h_block(rx, core, part=None):
        rows = pl.ds(pl.multiple_of((wrap(xx, rx) * 2 + core) * blk, 32), blk)
        return h_all.at[:, rows, :] if part is None else h_all.at[part, rows, :]

    def kv_block(rx, core, part=None):
        ref = kvx.at[wrap(xx, rx), core]
        return ref if part is None else ref.at[pl.ds(part * (seq // 2), seq // 2), :]

    def norm(layer):
        rows = pl.ds(pl.multiple_of(mi * blk, 32), blk)
        for b in range(batch):
            values = hid[b].astype(F32)
            centered = values - jnp.mean(values, axis=-1, keepdims=True)
            var = jnp.mean(centered * centered, axis=-1, keepdims=True)
            normed = centered * lax.rsqrt(var + EPS)
            for i in range(n_data):
                cols = slice(i * shard, (i + 1) * shard)
                h_all[b, rows, cols] = (normed[:, cols] * gbuf[i, layer:layer + 1, :]).astype(BF16)

    m_rows = seq // 2
    half_tiles = half_ff // head

    class Tile:
        def __init__(self, src, slot, pieces):
            self.copies = []
            at = 0
            for i, (start, n) in enumerate(pieces):
                self.copies.append(pltpu.make_async_copy(src.at[:, pl.ds(start, n)], wt.at[slot, :, pl.ds(at, n)], tsem.at[slot, i]))
                at += n

        def start(self):
            for copy in self.copies:
                copy.start()

        def wait(self):
            for copy in self.copies:
                copy.wait()

    def mlp_tile(layer, part, t, slot):
        src = (wi0 if part == 0 else wi1).at[layer]
        first = aligned((kvc + head if part == 0 else 0) + t * head, 128)
        return Tile(src, slot, ((first, head), (aligned(first + half_ff, 128), head)))

    def over_rows(fn):
        def body(i, carry):
            b = lax.div(i, 2)
            rows = pl.ds(pl.multiple_of(lax.rem(i, 2) * m_rows, m_rows), m_rows)
            fn(b, rows)
            return carry
        lax.fori_loop(0, 2 * batch, body, 0)

    def mlp(layer, part, begin, slot0, extra):
        blocks = 2 * batch

        def body(step, carry):
            t = lax.div(step, blocks)
            i = lax.rem(step, blocks)
            b = lax.div(i, 2)
            slot = lax.rem(t + slot0, 2)

            @pl.when(i == 0)
            def _():
                mlp_tile(layer, part, t, slot).wait()

            cols = pl.ds(pl.multiple_of(head + part * half_ff + t * head, head), head)
            for sub in range(m_rows // SUB):
                at = pl.ds(pl.multiple_of(lax.rem(i, 2) * m_rows + sub * SUB, SUB), SUB)
                res = dot(h_all[b, at, :], wt[slot])
                gate = res[:, :head].astype(BF16).astype(F32)
                up = res[:, head:].astype(BF16).astype(F32)
                joined[b, at, cols] = (gate * jax.nn.sigmoid(gate) * up).astype(BF16)

            @pl.when((i == blocks - 1) & (t + 2 < half_tiles))
            def _():
                mlp_tile(layer, part, t + 2, slot).start()

            for k in range(half_tiles * blocks):
                @pl.when(step == k)
                def _():
                    if k in extra:
                        extra[k]()
                    pump_until(begin + STEP * (k + 1))
            return carry

        lax.fori_loop(0, half_tiles * blocks, body, 0)

    def in_first(layer, kv, begin):
        kvq = Tile(wi0.at[layer], 0, ((0, kvc + head),))
        kvq.start()
        mlp_tile(layer, 0, 0, 1).start()
        kvq.wait()

        def do_kv(i, carry):
            rows = pl.ds(pl.multiple_of(i * m_rows, m_rows), m_rows)
            kvx[xx, cc, rows, :] = dot(h_all[cc, rows, :], wt[0, :, :kvc]).astype(BF16)
            return carry

        def do_q(b, rows):
            qb[b, rows, :] = dot(h_all[b, rows, :], wt[0, :, kvc:kvc + head]).astype(BF16)

        lax.fori_loop(0, 2, do_kv, 0)
        kv.start()
        pump_until(begin + 1)
        over_rows(do_q)
        mlp_tile(layer, 0, 1, 0).start()
        pump_until(begin + 3)

        mlp(layer, 0, begin + 3, 1, {5: kv.near, 9: kv.far})
        kv.rest()

    def in_second(layer, begin, then):
        mlp_tile(layer, 1, 0, 0).start()
        mlp_tile(layer, 1, 1, 1).start()
        mlp(layer, 1, begin, 0, {13: then})

    def wo_load(layer, k):
        return [pltpu.make_async_copy(woutb.at[layer, data_at(*BLOCKS[i])], wo.at[:, pl.ds(i * shard, shard)], osem.at[i])
                for i in range(*CHUNKS[k])]

    q_rows = 256

    def attention():
        def body(b, carry):
            for m in range(seq // q_rows):
                keys = (m + 1) * q_rows
                q = qb[b, m * q_rows:(m + 1) * q_rows, :]
                k = jnp.concatenate([kvx[0, b, :keys, :], kvx[1, b, :keys, :]], axis=-1)
                v = jnp.concatenate([kvx[2, b, :keys, :], kvx[3, b, :keys, :]], axis=-1)
                s = lax.dot_general(q, k, (((1,), (1,)), ((), ())), preferred_element_type=F32) * head ** -0.5
                row = lax.broadcasted_iota(jnp.int32, (q_rows, keys), 0) + m * q_rows
                col = lax.broadcasted_iota(jnp.int32, (q_rows, keys), 1)
                allowed = (col <= row) & (col < len_ref[b])
                s = jnp.where(allowed, s, NEG_BIG)
                e = jnp.exp(s - jnp.max(s, axis=-1, keepdims=True))
                p = e / jnp.sum(e, axis=-1, keepdims=True)
                o = dot(p, v.astype(F32))
                joined[b, m * q_rows:(m + 1) * q_rows, :head] = o.astype(BF16)
            return carry
        lax.fori_loop(0, batch, body, 0)

    PAIRS = (2, 1, -1, 0)
    pair_rows = 2 * blk

    def chunk_ds(k):
        first, last = CHUNKS[k]
        return pl.ds(first * shard, (last - first) * shard)

    def over_cols(k, fn):
        first, last = CHUNKS[k]

        def body(n, carry):
            fn(pl.ds(pl.multiple_of(first * shard + n * TILE, TILE), TILE))
            return carry
        lax.fori_loop(0, (last - first) * shard // TILE, body, 0)

    def out_proj(k, p):
        rows = pl.ds(pl.multiple_of(wrap(xx, PAIRS[p]) * pair_rows, 64), pair_rows)

        def fn(cols):
            lhs = joined[:, rows, :].reshape(batch * pair_rows, out_rows)
            res = dot(lhs, wo[:, cols]).astype(BF16)
            zp[p, :, :, cols] = res.reshape(batch, pair_rows, TILE)
        over_cols(k, fn)

    mine_rows = pl.ds(pl.multiple_of(cc * blk, 32), blk)
    other_rows = pl.ds(pl.multiple_of((1 - cc) * blk, 32), blk)

    class Scatter:
        def __init__(self, layer, k, out_ref):
            self.layer, self.k, self.out_ref, self.sent = layer, k, out_ref, []

        def send(self, idx, src, dst, dev):
            copy = remote(src, dst, rsend.at[self.layer, self.k, idx], rrecv.at[self.layer, self.k, idx], dev)
            copy.start()
            self.sent.append(copy)

        def wait(self, idx, dst):
            remote(dst, dst, rsend.at[self.layer, self.k, idx], rrecv.at[self.layer, self.k, idx], partner).wait_recv()

        def begin(self, p):
            here = chunk_ds(self.k)
            self.send(p, zp.at[p, :, other_rows, here], zrp.at[p, :, :, here], partner)

        def finish(self, p):
            k = self.k
            here = chunk_ds(k)

            def base(p, b, cols):
                return zp[p, b, mine_rows, cols].astype(F32) + zrp[p, b, :, cols].astype(F32)

            self.wait(p, zrp.at[p, :, :, here])
            if p == 0:
                def fn(cols):
                    for b in range(batch):
                        zs[0, b, :, cols] = base(0, b, cols).astype(BF16)
                over_cols(k, fn)
                self.send(4, zs.at[0, 0, :, here], xh.at[0, :, here], dev_x(1))
                self.send(5, zs.at[0, 1, :, here], xh.at[1, :, here], dev_x(-1))
            elif p < 3:
                self.wait(3 + p, xh.at[p - 1, :, here])

                def fn(cols):
                    for b in range(batch):
                        total = base(p, b, cols)
                        if b == p - 1:
                            total = total + xh[p - 1, :, cols].astype(F32)
                        zs[p, b, :, cols] = total.astype(BF16)
                over_cols(k, fn)
                self.send(5 + p, zs.at[p, :, :, here], xf.at[p - 1, :, :, here], dev_x(1 if p == 1 else -1))
            else:
                self.wait(6, xf.at[0, :, :, here])
                self.wait(7, xf.at[1, :, :, here])
                for b in range(batch):
                    for i in range(*CHUNKS[k]):
                        cols = slice(i * shard, (i + 1) * shard)
                        total = base(3, b, cols) + xf[0, b, :, cols].astype(F32) + xf[1, b, :, cols].astype(F32)
                        place = pl.ds(pl.multiple_of(data_at(*BLOCKS[i]) * shard, shard), shard)
                        self.out_ref[b, :, place] = (hid[b, :, place].astype(F32) + total).astype(BF16)

    for layer in BOTH:
        g = 3 * layer
        h = Gather(layer, 0, h_block)
        norm(layer)
        h.start()
        near, far, first, second, chunk_times = PHASES[layer]
        pump_until(near)
        h.near()
        pump_until(far)
        h.far()
        h.rest()
        pump_to(g)
        kv = Gather(layer, 1, kv_block)
        in_first(layer, kv, first)
        attention()
        pump_to(g + 1)
        loads = [wo_load(layer, k) for k in range(len(CHUNKS))]

        def load(k):
            pump_to(g + 2, CHUNK_EVENTS[k])
            for copy in wo_load(layer, k):
                copy.start()

        in_second(layer, second, lambda: load(0))
        h.drain()
        kv.drain()
        parts = [Scatter(layer, k, hid if layer == 0 else y_ref) for k in range(len(CHUNKS))]
        pending = []
        step = 0

        def settle(upto):
            for entry in sorted(pending):
                if entry[0] <= upto:
                    pending.remove(entry)
                    parts[entry[1]].finish(entry[2])

        for k, part in enumerate(parts):
            for copy in loads[k]:
                copy.wait()
            for p in range(4):
                out_proj(k, p)
                part.begin(p)
                pump_until(chunk_times[k] + p)
                pending.append((step + LAGS[p], k, p))
                step += 1
                settle(step)
            if part is not parts[-1]:
                if layer + k == 0:
                    settle(len(order))
                load(k + 1)
            else:
                pump_until(chunk_times[k] + 6)
        settle(len(order))
        for part in parts:
            for copy in part.sent:
                copy.wait_send()

    for build in drains:
        build().wait_send()


def solution(mesh):
    batch_spec = ('replica', 'data')
    model_size = mesh.shape['model']
    n_data = mesh.shape['data']
    ring = 4
    assert model_size == 2 * ring and n_data == ring * ring

    def device_body(x_in, lengths, norm_gain, w_in, w_kv, w_out):
        batch, blk, width = x_in.shape
        layers, shard, in_cols = w_in.shape
        out_rows = w_out.shape[1]
        head = w_kv.shape[-1] // 2
        seq = blk * model_size
        ff = out_rows - head
        kvc = 2 * head // ring
        vmem = pl.BlockSpec(memory_space=pltpu.VMEM)
        hbm = pl.BlockSpec(memory_space=pl.ANY)
        dma = pltpu.SemaphoreType.DMA
        groups = len(GROUPS)
        y = pl.pallas_call(
            lambda *refs: layer_kernel(ring, *refs),
            name='layers',
            out_shape=(
                jax.ShapeDtypeStruct(x_in.shape, BF16),
                jax.ShapeDtypeStruct((layers, width, kvc + head + ff), BF16),
                jax.ShapeDtypeStruct((layers, width, ff), BF16),
                jax.ShapeDtypeStruct((layers, n_data, out_rows, shard), BF16),
            ),
            in_specs=[vmem, pl.BlockSpec(memory_space=pltpu.SMEM)] + [vmem] * 4,
            out_specs=(vmem, hbm, hbm, hbm),
            scratch_shapes=[
                pltpu.VMEM((8, shard), F32),
                pltpu.VMEM((batch, seq, width), BF16),
                pltpu.VMEM((batch, seq, out_rows), BF16),
                pltpu.VMEM((ring, batch, seq, kvc), BF16),
                pltpu.VMEM((batch, seq, head), BF16),
                pltpu.VMEM((2, width, TILE), BF16),
                pltpu.VMEM((out_rows, width), BF16),
                pltpu.VMEM((4, batch, 2 * blk, width), BF16),
                pltpu.VMEM((4, batch, blk, width), BF16),
                pltpu.VMEM((2, blk, width), BF16),
                pltpu.VMEM((2, batch, blk, width), BF16),
                pltpu.VMEM((3, batch, blk, width), BF16),
                pltpu.VMEM((batch, blk, width), BF16),
                pltpu.VMEM((n_data, 8, shard), F32),
                dma((n_data,)), dma((n_data,)),
                dma((groups, 2, 16)), dma((groups, 2, 16)),
                dma((2, 2, 9)), dma((2, 2, 9)),
                dma((2, 3, 8)), dma((2, 3, 8)),
                dma((2, 6)), dma((2, 2)), dma((n_data,)),
            ],
            compiler_params=pltpu.CompilerParams(
                collective_id=0, has_side_effects=True, vmem_limit_bytes=67043328),
            cost_estimate=pl.CostEstimate(flops=90_000_000_000, bytes_accessed=200_000_000, transcendentals=0),
        )(x_in, lengths, norm_gain, w_in, w_kv, w_out)[0]
        return y

    in_specs = (P(batch_spec, 'model', None), P(batch_spec), P(None, 'data'), P(None, 'data', 'model'), P(None, 'data', None), P(None, 'model', 'data'))
    return jax.shard_map(device_body, mesh=mesh, in_specs=in_specs, out_specs=P(batch_spec, 'model', None), check_vma=False)
```
